32 devices in a mesh: dp: 2 (over y), expert: 4 (over z), tensor: 4 (over x, core).
Axes of the slice: x: 2, y: 2, z: 4, core: 2. Of those that a mesh axis runs over, the one named last changes fastest.
Arguments:
- grad_out: bfloat16 [1024, 6144], P(('dp', 'expert'), 'tensor'), may hold values from -0.1875 to 0.1875
- expert_ids: int32 [1024, 2], P(('dp', 'expert')), may hold values from 0 to 3, all different within a row; in each aligned block of 128 rows (0 to 127, 128 to 255, ...) at most 64 rows name the same one
- route_gates: float32 [1024, 2], P(('dp', 'expert')), may hold values from 0.1 to 1
- saved_hidden: bfloat16 [4, 256, 16384], P('expert', 'dp', 'tensor'), may hold values from -6 to 6
Outputs:
- weight_grad: bfloat16 [4, 16384, 6144], P('expert', 'tensor', 'dp')
The draws below stay inside these ranges and needn't reach their ends.
Inputs may be any that keep to these rules, and one draw needn't show every extreme that they name: `expert_ids`: each row names 2 different experts. Among the rows of one device no expert is named by more than 64 rows, and every expert is named somewhere.
All inputs are finite; a program needn't handle non-finite values.
Results may differ from the reference program's by a relative error of at most 0.0049.
Values may be sent and summed in bfloat16 or wider, within the bound.
A program may use at most 128 MiB of HBM per device.

```python
import math
import jax
import jax.numpy as jnp
import numpy as np
from jax import lax

D = 6144
FF = 16384
TOP = 2
TOK_DEV = 128
CAP = 32
EXPERTS = 4
TOKENS = 1024
SLOTS = 256
N_DP = 2


def block_scale(key, dims, cuts, smallest, high):
    def one(position, shards_of):
        draws = jax.random.uniform(jax.random.fold_in(jax.random.fold_in(key, 6), position), (shards_of,), jnp.float32, smallest / len(cuts), high / len(cuts))
        return jnp.repeat(jnp.exp(draws), dims[position] // shards_of).reshape((-1,) + (1,) * (len(dims) - position - 1))

    gain = one(*cuts[0])
    for cut in cuts[1:]:
        gain = gain * one(*cut)
    return gain


def deal_out(own_key, own, number, rows, amount, top, most, lean):
    sequence = jax.random.permutation(own_key, amount)
    heavy_load, common = shares(amount, rows * top, most, lean, True), shares(amount, rows * top, most, lean, False)
    places = jnp.arange(amount)

    def named(sizes, rotation):
        used = int((sizes > 0).sum())
        fixed = max(1, used // 4)
        moved = fixed + (places - fixed + rotation * (used - fixed)) % max(1, amount - fixed)
        return jnp.zeros((amount,), jnp.int32).at[sequence[jnp.where(places < fixed, places, moved)]].set(jnp.asarray(sizes, jnp.int32))

    sizes = jnp.where(number % 4 == 0, named(heavy_load, number // 4), named(common, number - number // 4 - 1))
    mixed = jax.random.permutation(jax.random.fold_in(own, 3), amount)
    donor, taker = mixed[0:amount // 2 * 2:2], mixed[1:amount // 2 * 2:2]
    margin = jnp.minimum(sizes[donor] - 1, most - sizes[taker]) // 2
    margin = jnp.where((donor == sequence[0]) | (taker == sequence[0]) | (sizes[taker] == 0), 0, jnp.maximum(margin, 0))
    moved = jax.random.randint(jax.random.fold_in(own, 4), (amount // 2,), 0, 1 << 20) % (margin + 1)
    sizes = sizes.at[donor].add(-moved).at[taker].add(moved)
    members = jnp.searchsorted(jnp.cumsum(sizes), jnp.arange(rows * top), side="right").astype(jnp.int32)
    listing = members.reshape(top, rows).T
    listing = listing[jax.random.permutation(jax.random.fold_in(own, 1), rows)]
    rotation = jax.random.randint(jax.random.fold_in(own, 2), (rows, 1), 0, top)
    return jnp.take_along_axis(listing, (jnp.arange(top)[None, :] + rotation) % top, axis=1)


def shares(count, total, limit, lean, full):
    loads = [(1 << 20) // math.isqrt(rank ** lean) + 1 for rank in range(1, count + 1)]
    largest = limit if full else min(limit, max(-(-total // count), total * loads[0] // sum(loads)))
    least = 1 if total - largest >= count - 1 else 0
    counts, spare = [largest] + [least] * (count - 1), total - largest - least * (count - 1)
    while spare > 0:
        free = [i for i in range(1, count) if counts[i] < largest] or [i for i in range(1, count) if counts[i] < limit]
        whole, remaining = sum([loads[i] for i in free]), spare
        for i in free:
            more = min(limit - counts[i], max(1, remaining * loads[i] // whole), spare)
            counts[i] = counts[i] + more
            spare = spare - more
    return np.array(counts)


def centred(stream_key, extent, width, bound, cuts=(), kind=jnp.bfloat16):
    factor_of = block_scale(stream_key, extent, cuts, -0.22, 0.18) if cuts else 1.0
    result = jax.random.normal(stream_key, extent, jnp.float32) * width * factor_of
    return jnp.minimum(jnp.maximum(result, -bound), bound).astype(kind)


def setup_inputs(seed: int = 0) -> dict:
    arg_keys = jax.random.split(jax.random.key(seed), 5)
    grad_out = centred(arg_keys[0], (TOKENS, D), 0.03, 0.1875, ((0, 8), (1, 4)))
    expert_ids_keys = jax.random.split(jax.random.fold_in(arg_keys[1], 1), TOKENS // TOK_DEV)
    expert_ids_turns = jax.random.permutation(jax.random.fold_in(arg_keys[1], 3), TOKENS // TOK_DEV)
    expert_ids = jax.vmap(lambda own, number: deal_out(jax.random.fold_in(arg_keys[1], 2), own, number, TOK_DEV, EXPERTS, TOP, TOK_DEV // 2, 2))(expert_ids_keys, expert_ids_turns).reshape((TOKENS, TOP))
    route_gates = jnp.clip(0.1 + 0.9 * jax.random.uniform(arg_keys[2], (TOKENS, TOP), jnp.float32) ** block_scale(arg_keys[2], (TOKENS, TOP), ((0, 8),), -0.2, 0.2), 0.1, 1.0)
    saved_hidden = centred(arg_keys[3], (EXPERTS, SLOTS, FF), 1.0, 6.0, ((0, 4), (1, 2), (2, 4)))
    return dict(grad_out=grad_out, expert_ids=expert_ids, route_gates=route_gates, saved_hidden=saved_hidden)


def slot_table(expert_ids, route_gates, expert_count):
    routes = expert_ids.reshape(-1).astype(jnp.int32)
    weights = route_gates.reshape(-1)
    onehot = (routes[:, None] == jnp.arange(expert_count, dtype=jnp.int32)[None, :]).astype(jnp.int32)
    before = jnp.cumsum(onehot, axis=0) - onehot
    rank = jnp.sum(before * onehot, axis=1)
    target = jnp.where(rank < CAP, routes * CAP + rank, -1)
    match = jnp.arange(expert_count * CAP, dtype=jnp.int32)[:, None] == target[None, :]
    chosen = match.reshape(expert_count * CAP, -1, TOP).any(axis=2)
    slot_gate = jnp.sum(jnp.where(match, weights[None, :], jnp.zeros_like(weights)[None, :]), axis=1)
    return chosen.astype(jnp.bfloat16), slot_gate


def reference(grad_out, expert_ids, route_gates, saved_hidden):
    blocks = N_DP * EXPERTS
    grads = grad_out.reshape(blocks, TOK_DEV, D)
    ids = expert_ids.reshape(blocks, TOK_DEV, TOP)
    gates = route_gates.reshape(blocks, TOK_DEV, TOP)

    def one_block(items):
        grad_block, id_block, gate_block = items
        chosen, slot_gate = slot_table(id_block, gate_block, EXPERTS)
        picked = jnp.dot(chosen, grad_block, preferred_element_type=jnp.float32)
        return (picked * slot_gate[:, None]).astype(jnp.bfloat16).reshape(EXPERTS, CAP, D)

    slots = lax.map(one_block, (grads, ids, gates))
    slots = jnp.transpose(slots, (1, 0, 2, 3)).reshape(EXPERTS, blocks * CAP, D)

    def one_expert(items):
        hidden, expert_grads = items
        summed = lax.dot_general(hidden, expert_grads, (((0,), (0,)), ((), ())), preferred_element_type=jnp.float32)
        return summed.astype(jnp.bfloat16)

    return lax.map(one_expert, (saved_hidden, slots))
```

```python
import functools

import jax
import jax.numpy as jnp
from jax import lax
from jax.experimental import pallas as pl
from jax.experimental.pallas import tpu as pltpu
from jax.sharding import PartitionSpec as P

TOP = 2
CAP = 32
MESH = pl.DeviceIdType.MESH
TN = (((0,), (0,)), ((), ()))


def slot_table(expert_ids, route_gates, expert_count):
    routes = expert_ids.reshape(-1)
    weights = route_gates.reshape(-1)
    onehot = (routes[:, None] == jnp.arange(expert_count, dtype=jnp.int32)[None, :]).astype(
        jnp.int32
    )
    before = jnp.cumsum(onehot, axis=0) - onehot
    rank = jnp.sum(before * onehot, axis=1)
    target = jnp.where(rank < CAP, routes * CAP + rank, -1)
    match = jnp.arange(expert_count * CAP, dtype=jnp.int32)[:, None] == target[None, :]
    chosen = match.reshape(expert_count * CAP, -1, TOP).any(axis=2)
    slot_gate = jnp.sum(
        jnp.where(match, weights[None, :], jnp.zeros_like(weights)[None, :]), axis=1
    )
    return (chosen.astype(jnp.bfloat16), slot_gate)


def plain(grad_out, expert_ids, route_gates, saved_hidden):
    data_count = lax.axis_size("dp")
    expert_count = lax.axis_size("expert")
    chosen, slot_gate = slot_table(expert_ids, route_gates, expert_count)
    width = grad_out.shape[1] * lax.axis_size("tensor")
    block_width = width // data_count
    complete = lax.all_gather(grad_out, "tensor", axis=1, tiled=True)
    parted = complete.reshape(complete.shape[0], data_count, block_width)
    picked = jnp.einsum("st,tdk->dsk", chosen, parted, preferred_element_type=jnp.float32)
    outgoing = (picked * slot_gate[None, :, None]).astype(jnp.bfloat16)
    outgoing = outgoing.reshape(data_count * expert_count, CAP, block_width)
    arrived = lax.all_to_all(outgoing, ("dp", "expert"), split_axis=0, concat_axis=0, tiled=True)
    received = arrived.reshape(-1, block_width)
    summed = lax.dot_general(
        lax.all_gather(saved_hidden[0], "dp", axis=0, tiled=True),
        received,
        TN,
        preferred_element_type=jnp.float32,
    )
    return summed.astype(jnp.bfloat16)[None]


def slot_rows(ids, gates, grad, experts):
    tokens = ids.shape[1]
    named, gate, rank = [], [], []
    for e in range(experts):
        first = (ids[0:1, :] == e).astype(jnp.float32)
        second = (ids[1:2, :] == e).astype(jnp.float32)
        named.append(jnp.broadcast_to(first + second, (CAP, tokens)))
        gate.append(jnp.broadcast_to(first * gates[0:1, :] + second * gates[1:2, :], (CAP, tokens)))
        rank.append(lax.broadcasted_iota(jnp.int32, (CAP, tokens), 0))
    named = jnp.concatenate(named, axis=0)
    gate = jnp.concatenate(gate, axis=0)
    rank = jnp.concatenate(rank, axis=0).astype(jnp.float32)
    row = lax.broadcasted_iota(jnp.int32, (tokens, tokens), 0)
    column = lax.broadcasted_iota(jnp.int32, (tokens, tokens), 1)
    earlier = jnp.where(row < column, 1.0, 0.0).astype(jnp.bfloat16)
    before = jnp.dot(named.astype(jnp.bfloat16), earlier, preferred_element_type=jnp.float32)
    chosen = jnp.where(before == rank, named, 0.0)
    slot_gate = jnp.sum(chosen * gate, axis=1, keepdims=True)
    picked = jnp.dot(chosen.astype(jnp.bfloat16), grad, preferred_element_type=jnp.float32)
    return (picked * slot_gate).astype(jnp.bfloat16)


def exchange(
    D, E, T, cuts, ids_ref, gates_ref, grad_ref, hidden_ref, g_ref, other_ref, slots,
    h_send, h_recv, s1, r1, s2, r2, s3, r3,
):
    d, e, t = lax.axis_index("dp"), lax.axis_index("expert"), lax.axis_index("tensor")
    q = T // D
    x, c = t // q, t % q
    cols = grad_ref.shape[1]
    W = cols // D
    rows = hidden_ref.shape[0]

    def hidden_copy(n, i):
        lo, hi = cuts[i], cuts[i + 1]
        return pltpu.make_async_remote_copy(
            src_ref=hidden_ref.at[pl.ds(lo, hi - lo), :],
            dst_ref=other_ref.at[pl.ds((D - n - 1) * rows + lo, hi - lo), :],
            send_sem=h_send.at[n - 1, i],
            recv_sem=h_recv.at[D - n - 1, i],
            device_id=((d + n) % D, e, t),
            device_id_type=MESH,
        )

    barrier = pltpu.get_barrier_semaphore()

    def greet(to):
        pl.semaphore_signal(barrier, inc=1, device_id=to, device_id_type=MESH)

    for n in range(1, D):
        greet(((d + n) % D, e, t))
        greet((d, e, ((x + n) % D) * q + c))
    for p in range(1, q):
        greet((d, e, x * q + (c + p) % q))
    for n in range(D):
        for j in range(E):
            to = ((x + n) % D, (e + j) % E, d * q + c)
            if n == 0 and j == 0:
                pl.when(x != d)(functools.partial(greet, to))
            else:
                greet(to)
    slots[...] = slot_rows(ids_ref[...], gates_ref[...], grad_ref[...], E)
    pl.semaphore_wait(barrier, 2 * (D - 1) + q - 1 + D * E - jnp.where(x == d, 1, 0))

    for n in range(1, D):
        hidden_copy(n, 0).start()

    def place(r, source, x_at, c_at):
        return g_ref.at[
            pl.ds(pl.multiple_of(r * (E * CAP) + source * CAP, CAP), CAP),
            pl.ds(pl.multiple_of(c_at * cols + x_at * W, 128), W),
        ]

    def first(j, m):
        e2, x2 = (e + j) % E, (x + m) % D
        r = (d - x + D) % D
        src = slots.at[
            pl.ds(pl.multiple_of(e2 * CAP, CAP), CAP), pl.ds(pl.multiple_of(x2 * W, 128), W)
        ]
        return src, place(r, e, x2, c), r1.at[r, (E - j) % E], (x, e2, x2 * q + c)

    def first_remote(j, m):
        src, dst, sem, to = first(j, m)
        return pltpu.make_async_remote_copy(
            src_ref=src, dst_ref=dst, send_sem=s1.at[j, m], recv_sem=sem,
            device_id=to, device_id_type=MESH,
        )

    def first_local():
        src = slots.at[
            pl.ds(pl.multiple_of(e * CAP, CAP), CAP), pl.ds(pl.multiple_of(x * W, 128), W)
        ]
        return pltpu.make_async_copy(src, place(0, e, x, c), r1.at[0, 0])

    order = sorted(range(E), key=lambda j: -min(j, E - j))
    for j in order:
        for m in range(D):
            if j == 0 and m == 0:
                pl.when(x == d)(lambda: first_local().start())
                pl.when(x != d)(lambda: first_remote(0, 0).start())
            else:
                first_remote(j, m).start()

    for i in range(1, len(cuts) - 1):
        for n in range(1, D):
            hidden_copy(n, i).start()

    def along(n, r, k):
        here = place(r, (e + k) % E, x, c)
        return pltpu.make_async_remote_copy(
            src_ref=here, dst_ref=here, send_sem=s2.at[n - 1, r, k], recv_sem=r2.at[D - n - 1, r, k],
            device_id=(d, e, ((x + n) % D) * q + c), device_id_type=MESH,
        )

    def along_arrived(n, r, k):
        here = place(r, (e + k) % E, (x + n) % D, c)
        return pltpu.make_async_remote_copy(
            src_ref=here, dst_ref=here, send_sem=s2.at[n - 1, r, k], recv_sem=r2.at[n - 1, r, k],
            device_id=(d, e, ((x + n) % D) * q + c), device_id_type=MESH,
        )

    def across(p, n, r, k):
        here = place(r, (e + k) % E, (x + n) % D, c)
        return pltpu.make_async_remote_copy(
            src_ref=here, dst_ref=here, send_sem=s3.at[p - 1, n, r, k],
            recv_sem=r3.at[q - p - 1, n, r, k],
            device_id=(d, e, x * q + (c + p) % q), device_id_type=MESH,
        )

    def across_arrived(p, n, r, k):
        here = place(r, (e + k) % E, (x + n) % D, (c + p) % q)
        return pltpu.make_async_remote_copy(
            src_ref=here, dst_ref=here, send_sem=s3.at[p - 1, n, r, k],
            recv_sem=r3.at[p - 1, n, r, k],
            device_id=(d, e, x * q + (c + p) % q), device_id_type=MESH,
        )

    def first_arrived(r, k):
        here = place(r, (e + k) % E, x, c)
        return pltpu.make_async_remote_copy(
            src_ref=here, dst_ref=here, send_sem=s1.at[0, 0], recv_sem=r1.at[r, k],
            device_id=((d + r) % D, (e + k) % E, d * q + c), device_id_type=MESH,
        )

    blocks = [(r, k) for k in reversed(order) for r in range(D)]
    for r, k in blocks:
        if r == 0 and k == 0:
            pl.when(x == d)(lambda: first_local().wait())
            pl.when(x != d)(lambda: first_arrived(0, 0).wait_recv())
        else:
            first_arrived(r, k).wait_recv()
        for n in range(1, D):
            along(n, r, k).start()
        for p in range(1, q):
            across(p, 0, r, k).start()
    for r, k in blocks:
        for n in range(1, D):
            along_arrived(n, r, k).wait_recv()
            for p in range(1, q):
                across(p, n, r, k).start()
    for r, k in blocks:
        for p in range(1, q):
            for n in range(D):
                across_arrived(p, n, r, k).wait_recv()
    for j in order:
        for m in range(D):
            if j == 0 and m == 0:
                pl.when(x != d)(lambda: first_remote(0, 0).wait_send())
            else:
                first_remote(j, m).wait_send()
    for r, k in blocks:
        for n in range(1, D):
            along(n, r, k).wait_send()
        for p in range(1, q):
            for n in range(D):
                across(p, n, r, k).wait_send()
    for i in range(len(cuts) - 1):
        for n in range(1, D):
            hidden_copy(n, i).wait_send()
            pltpu.make_async_remote_copy(
                src_ref=hidden_ref.at[pl.ds(cuts[i], cuts[i + 1] - cuts[i]), :],
                dst_ref=other_ref.at[pl.ds((n - 1) * rows + cuts[i], cuts[i + 1] - cuts[i]), :],
                send_sem=h_send.at[n - 1, i],
                recv_sem=h_recv.at[n - 1, i],
                device_id=((d + n) % D, e, t),
                device_id_type=MESH,
            ).wait_recv()


def product(strip, own_ref, other_ref, g_ref, o_ref):
    hidden = jnp.concatenate([own_ref[...], other_ref[...]], axis=0)
    for lo in range(0, g_ref.shape[1], strip):
        o_ref[:, lo:lo + strip] = lax.dot_general(
            hidden, g_ref[:, lo:lo + strip], TN, preferred_element_type=jnp.float32
        ).astype(o_ref.dtype)


def local(grad_out, expert_ids, route_gates, saved_hidden):
    D, E, T = lax.axis_size("dp"), lax.axis_size("expert"), lax.axis_size("tensor")
    tokens, cols = grad_out.shape
    rows, units = saved_hidden.shape[1:]
    depth = D * E * CAP
    width = cols * T // D
    tile, strip = 1024, 1024
    if T % D or cols % (128 * D) or units % tile or width % strip or rows != E * CAP or tokens % 128:
        return plain(grad_out, expert_ids, route_gates, saved_hidden)
    q = T // D
    hidden = saved_hidden[0]
    cuts = (0, rows // 4, rows)
    pieces = len(cuts) - 1
    vmem = pl.BlockSpec(memory_space=pltpu.VMEM)
    hbm = pl.BlockSpec(memory_space=pl.ANY)
    dma = pltpu.SemaphoreType.DMA
    g, other = pl.pallas_call(
        functools.partial(exchange, D, E, T, cuts),
        out_shape=(
            jax.ShapeDtypeStruct((depth, width), jnp.bfloat16),
            jax.ShapeDtypeStruct(((D - 1) * rows, units), jnp.bfloat16),
        ),
        in_specs=[vmem, vmem, vmem, hbm],
        out_specs=(vmem, hbm),
        scratch_shapes=[
            pltpu.VMEM((E * CAP, cols), jnp.bfloat16),
            dma((D - 1, pieces)), dma((D - 1, pieces)),
            dma((E, D)), dma((D, E)),
            dma((D - 1, D, E)), dma((D - 1, D, E)),
            dma((q - 1, D, D, E)), dma((q - 1, D, D, E)),
        ],
        compiler_params=pltpu.CompilerParams(has_side_effects=True, collective_id=0),
    )(expert_ids.T, route_gates.T, grad_out, hidden)
    summed = pl.pallas_call(
        functools.partial(product, strip),
        grid=(units // tile,),
        out_shape=jax.ShapeDtypeStruct((units, width), jnp.bfloat16),
        in_specs=[
            pl.BlockSpec((rows, tile), lambda i: (0, i)),
            pl.BlockSpec(((D - 1) * rows, tile), lambda i: (0, i)),
            pl.BlockSpec((depth, width), lambda i: (0, 0)),
        ],
        out_specs=pl.BlockSpec((tile, width), lambda i: (i, 0)),
        compiler_params=pltpu.CompilerParams(dimension_semantics=("arbitrary",)),
    )(hidden, other, g)
    return summed[None]


def solution(mesh):
    in_specs = (
        P(("dp", "expert"), "tensor"),
        P(("dp", "expert"), None),
        P(("dp", "expert"), None),
        P("expert", "dp", "tensor"),
    )
    out_specs = P("expert", "tensor", "dp")
    return jax.shard_map(local, mesh=mesh, in_specs=in_specs, out_specs=out_specs, check_vma=False)
```

```python
import functools

import jax
import jax.numpy as jnp
from jax import lax
from jax.experimental import pallas as pl
from jax.experimental.pallas import tpu as pltpu
from jax.sharding import PartitionSpec as P

TOP = 2
CAP = 32
MESH = pl.DeviceIdType.MESH
TN = (((0,), (0,)), ((), ()))
EARLY, INSIDE, LATER = 1, 4, (2, 1, 1)


def slot_table(expert_ids, route_gates, expert_count):
    routes = expert_ids.reshape(-1)
    weights = route_gates.reshape(-1)
    onehot = (routes[:, None] == jnp.arange(expert_count, dtype=jnp.int32)[None, :]).astype(
        jnp.int32
    )
    before = jnp.cumsum(onehot, axis=0) - onehot
    rank = jnp.sum(before * onehot, axis=1)
    target = jnp.where(rank < CAP, routes * CAP + rank, -1)
    match = jnp.arange(expert_count * CAP, dtype=jnp.int32)[:, None] == target[None, :]
    chosen = match.reshape(expert_count * CAP, -1, TOP).any(axis=2)
    slot_gate = jnp.sum(
        jnp.where(match, weights[None, :], jnp.zeros_like(weights)[None, :]), axis=1
    )
    return (chosen.astype(jnp.bfloat16), slot_gate)


def plain(grad_out, expert_ids, route_gates, saved_hidden):
    data_count = lax.axis_size("dp")
    expert_count = lax.axis_size("expert")
    chosen, slot_gate = slot_table(expert_ids, route_gates, expert_count)
    width = grad_out.shape[1] * lax.axis_size("tensor")
    block_width = width // data_count
    complete = lax.all_gather(grad_out, "tensor", axis=1, tiled=True)
    parted = complete.reshape(complete.shape[0], data_count, block_width)
    picked = jnp.einsum("st,tdk->dsk", chosen, parted, preferred_element_type=jnp.float32)
    outgoing = (picked * slot_gate[None, :, None]).astype(jnp.bfloat16)
    outgoing = outgoing.reshape(data_count * expert_count, CAP, block_width)
    arrived = lax.all_to_all(outgoing, ("dp", "expert"), split_axis=0, concat_axis=0, tiled=True)
    received = arrived.reshape(-1, block_width)
    summed = lax.dot_general(
        lax.all_gather(saved_hidden[0], "dp", axis=0, tiled=True),
        received,
        TN,
        preferred_element_type=jnp.float32,
    )
    return summed.astype(jnp.bfloat16)[None]


def slot_rows(ids, gates, grad, experts):
    tokens = ids.shape[1]
    named, gate, rank = [], [], []
    for e in range(experts):
        first = (ids[0:1, :] == e).astype(jnp.float32)
        second = (ids[1:2, :] == e).astype(jnp.float32)
        named.append(jnp.broadcast_to(first + second, (CAP, tokens)))
        gate.append(jnp.broadcast_to(first * gates[0:1, :] + second * gates[1:2, :], (CAP, tokens)))
        rank.append(lax.broadcasted_iota(jnp.int32, (CAP, tokens), 0))
    named = jnp.concatenate(named, axis=0)
    gate = jnp.concatenate(gate, axis=0)
    rank = jnp.concatenate(rank, axis=0).astype(jnp.float32)
    row = lax.broadcasted_iota(jnp.int32, (tokens, tokens), 0)
    column = lax.broadcasted_iota(jnp.int32, (tokens, tokens), 1)
    earlier = jnp.where(row < column, 1.0, 0.0).astype(jnp.bfloat16)
    before = jnp.dot(named.astype(jnp.bfloat16), earlier, preferred_element_type=jnp.float32)
    chosen = jnp.where(before == rank, named, 0.0)
    slot_gate = jnp.sum(chosen * gate, axis=1, keepdims=True)
    picked = jnp.dot(chosen.astype(jnp.bfloat16), grad, preferred_element_type=jnp.float32)
    return (picked * slot_gate).astype(jnp.bfloat16)


def exchange(
    D, E, T, lo, hi, later, ids_ref, gates_ref, grad_ref, hidden_ref, g_ref, other_ref, *rest
):
    parts = rest[:len(later)]
    (slots, staged, p_in, p_out, h_send, h_recv, s1, r1, s2, r2, s3, r3) = rest[len(later):]
    d, e, t = lax.axis_index("dp"), lax.axis_index("expert"), lax.axis_index("tensor")
    q = T // D
    x, c = t // q, t % q
    cols = grad_ref.shape[1]
    W = cols // D

    def hidden_copy():
        return pltpu.make_async_remote_copy(
            src_ref=hidden_ref.at[:, pl.ds(lo, hi - lo)],
            dst_ref=other_ref,
            send_sem=h_send,
            recv_sem=h_recv,
            device_id=((d + 1) % D, e, t),
            device_id_type=MESH,
        )

    def stage_in(i):
        at, size = later[i]
        return pltpu.make_async_copy(
            hidden_ref.at[:, pl.ds(at, size)], staged.at[:, pl.ds(at - hi, size)], p_in.at[i]
        )

    def stage_out(i):
        at, size = later[i]
        return pltpu.make_async_copy(staged.at[:, pl.ds(at - hi, size)], parts[i], p_out.at[i])

    barrier = pltpu.get_barrier_semaphore()

    def greet(to):
        pl.semaphore_signal(barrier, inc=1, device_id=to, device_id_type=MESH)

    for n in range(1, D):
        greet(((d + n) % D, e, t))
        greet((d, e, ((x + n) % D) * q + c))
    for p in range(1, q):
        greet((d, e, x * q + (c + p) % q))
    for n in range(D):
        for j in range(E):
            to = ((x + n) % D, (e + j) % E, d * q + c)
            if n == 0 and j == 0:
                pl.when(x != d)(functools.partial(greet, to))
            else:
                greet(to)
    for i in range(len(later)):
        stage_in(i).start()
    slots[...] = slot_rows(ids_ref[...], gates_ref[...], grad_ref[...], E)
    pl.semaphore_wait(barrier, 2 * (D - 1) + q - 1 + D * E - jnp.where(x == d, 1, 0))

    def place(r, source, x_at, c_at):
        return g_ref.at[
            pl.ds(pl.multiple_of(r * (E * CAP) + source * CAP, CAP), CAP),
            pl.ds(pl.multiple_of(c_at * cols + x_at * W, 128), W),
        ]

    def first(j, m):
        e2, x2 = (e + j) % E, (x + m) % D
        r = (d - x + D) % D
        src = slots.at[
            pl.ds(pl.multiple_of(e2 * CAP, CAP), CAP), pl.ds(pl.multiple_of(x2 * W, 128), W)
        ]
        return src, place(r, e, x2, c), r1.at[r, (E - j) % E], (x, e2, x2 * q + c)

    def first_remote(j, m):
        src, dst, sem, to = first(j, m)
        return pltpu.make_async_remote_copy(
            src_ref=src, dst_ref=dst, send_sem=s1.at[j, m], recv_sem=sem,
            device_id=to, device_id_type=MESH,
        )

    def first_local():
        src = slots.at[
            pl.ds(pl.multiple_of(e * CAP, CAP), CAP), pl.ds(pl.multiple_of(x * W, 128), W)
        ]
        return pltpu.make_async_copy(src, place(0, e, x, c), r1.at[0, 0])

    order = sorted(range(E), key=lambda j: -min(j, E - j))
    for j in order:
        for m in range(D):
            if j == 0 and m == 0:
                pl.when(x == d)(lambda: first_local().start())
                pl.when(x != d)(lambda: first_remote(0, 0).start())
            else:
                first_remote(j, m).start()

    hidden_copy().start()
    for i in range(len(later)):
        stage_in(i).wait()
        stage_out(i).start()

    def along(n, r, k):
        here = place(r, (e + k) % E, x, c)
        return pltpu.make_async_remote_copy(
            src_ref=here, dst_ref=here, send_sem=s2.at[n - 1, r, k], recv_sem=r2.at[D - n - 1, r, k],
            device_id=(d, e, ((x + n) % D) * q + c), device_id_type=MESH,
        )

    def along_arrived(n, r, k):
        here = place(r, (e + k) % E, (x + n) % D, c)
        return pltpu.make_async_remote_copy(
            src_ref=here, dst_ref=here, send_sem=s2.at[n - 1, r, k], recv_sem=r2.at[n - 1, r, k],
            device_id=(d, e, ((x + n) % D) * q + c), device_id_type=MESH,
        )

    def across(p, n, r, k):
        here = place(r, (e + k) % E, (x + n) % D, c)
        return pltpu.make_async_remote_copy(
            src_ref=here, dst_ref=here, send_sem=s3.at[p - 1, n, r, k],
            recv_sem=r3.at[q - p - 1, n, r, k],
            device_id=(d, e, x * q + (c + p) % q), device_id_type=MESH,
        )

    def across_arrived(p, n, r, k):
        here = place(r, (e + k) % E, (x + n) % D, (c + p) % q)
        return pltpu.make_async_remote_copy(
            src_ref=here, dst_ref=here, send_sem=s3.at[p - 1, n, r, k],
            recv_sem=r3.at[p - 1, n, r, k],
            device_id=(d, e, x * q + (c + p) % q), device_id_type=MESH,
        )

    def first_arrived(r, k):
        here = place(r, (e + k) % E, x, c)
        return pltpu.make_async_remote_copy(
            src_ref=here, dst_ref=here, send_sem=s1.at[0, 0], recv_sem=r1.at[r, k],
            device_id=((d + r) % D, (e + k) % E, d * q + c), device_id_type=MESH,
        )

    blocks = [(r, k) for k in reversed(order) for r in range(D)]
    for r, k in blocks:
        if r == 0 and k == 0:
            pl.when(x == d)(lambda: first_local().wait())
            pl.when(x != d)(lambda: first_arrived(0, 0).wait_recv())
        else:
            first_arrived(r, k).wait_recv()
        for n in range(1, D):
            along(n, r, k).start()
        for p in range(1, q):
            across(p, 0, r, k).start()
    for r, k in blocks:
        for n in range(1, D):
            along_arrived(n, r, k).wait_recv()
            for p in range(1, q):
                across(p, n, r, k).start()
    for r, k in blocks:
        for p in range(1, q):
            for n in range(D):
                across_arrived(p, n, r, k).wait_recv()
    for j in order:
        for m in range(D):
            if j == 0 and m == 0:
                pl.when(x != d)(lambda: first_remote(0, 0).wait_send())
            else:
                first_remote(j, m).wait_send()
    for r, k in blocks:
        for n in range(1, D):
            along(n, r, k).wait_send()
        for p in range(1, q):
            for n in range(D):
                across(p, n, r, k).wait_send()
    for i in range(len(later)):
        stage_out(i).wait()
    hidden_copy().wait()


def product(base, spans, tile, strip, slots, own_ref, *refs):
    others = refs[:len(spans)]
    g_ref = refs[len(spans)]
    o_ref, hv, gv, ob, hs, gs, os = refs[-7:]
    rows, width = own_ref.shape[0], g_ref.shape[1]
    tiles = [(o, at) for o, size in zip(others, spans) for at in range(0, size, tile)]
    count = len(tiles)
    depth = min(slots, count)

    def load(k):
        other, at = tiles[k]
        return (
            pltpu.make_async_copy(
                own_ref.at[:, pl.ds(base + k * tile, tile)], hv.at[k, pl.ds(0, rows), :], hs.at[k, 0]
            ),
            pltpu.make_async_copy(
                other.at[:, pl.ds(at, tile)], hv.at[k, pl.ds(rows, rows), :], hs.at[k, 1]
            ),
        )

    def loaded(k):
        for i in range(2):
            pltpu.make_async_copy(
                own_ref.at[:, pl.ds(0, tile)], hv.at[k, pl.ds(i * rows, rows), :], hs.at[k, i]
            ).wait()

    pieces = [
        pltpu.make_async_copy(g_ref.at[:, pl.ds(at, strip)], gv.at[:, pl.ds(at, strip)], gs.at[i])
        for i, at in enumerate(range(0, width, strip))
    ]
    for k in range(count):
        for copy in load(k):
            copy.start()
        if k == 0:
            for copy in pieces:
                copy.start()

    def leave(k):
        return pltpu.make_async_copy(
            ob.at[k % depth],
            o_ref.at[pl.ds(pl.multiple_of(base + k * tile, tile), tile), :],
            os.at[k % depth],
        )

    def step(k, opening=False, reuse=False):
        loaded(k)
        if reuse:
            leave(k - depth).wait()
        hidden = hv[k]
        for i, at in enumerate(range(0, width, strip)):
            if opening:
                pieces[i].wait()
            ob[k % depth, :, at:at + strip] = lax.dot_general(
                hidden, gv[:, at:at + strip], TN, preferred_element_type=jnp.float32
            ).astype(ob.dtype)
        leave(k).start()

    step(0, opening=True)
    if depth > 1:
        pl.loop(1, depth)(lambda k: step(k))
    if count > depth:
        pl.loop(depth, count)(lambda k: step(k, reuse=True))
    for k in range(count - depth, count):
        leave(k).wait()


def local(grad_out, expert_ids, route_gates, saved_hidden):
    D, E, T = lax.axis_size("dp"), lax.axis_size("expert"), lax.axis_size("tensor")
    tokens, cols = grad_out.shape
    rows, units = saved_hidden.shape[1:]
    depth = D * E * CAP
    width = cols * T // D
    tile, strip = 512, 1024
    if (
        D != 2 or T % D or cols % (128 * D) or units % (8 * tile) or width % strip
        or rows != E * CAP or tokens % 128
    ):
        return plain(grad_out, expert_ids, route_gates, saved_hidden)
    q = T // D
    hidden = saved_hidden[0]
    share = units // 8
    ahead, stop = EARLY * share, INSIDE * share
    later, at = [], stop
    for part in LATER:
        later.append((at, part * share))
        at += part * share
    later = tuple(later)
    vmem = pl.BlockSpec(memory_space=pltpu.VMEM)
    hbm = pl.BlockSpec(memory_space=pl.ANY)
    dma = pltpu.SemaphoreType.DMA
    bf16 = jnp.bfloat16
    swap = [(0, 1), (1, 0)]
    first = lax.ppermute(hidden[:, :ahead], "dp", swap)
    g, other, *parts = pl.pallas_call(
        functools.partial(exchange, D, E, T, ahead, stop, later),
        out_shape=(
            jax.ShapeDtypeStruct((depth, width), bf16),
            jax.ShapeDtypeStruct((rows, stop - ahead), bf16),
            *(jax.ShapeDtypeStruct((rows, size), bf16) for _, size in later),
        ),
        in_specs=[vmem, vmem, vmem, hbm],
        out_specs=(vmem, hbm, *(hbm for _ in later)),
        scratch_shapes=[
            pltpu.VMEM((E * CAP, cols), bf16),
            pltpu.VMEM((rows, units - stop), bf16),
            dma((len(later),)), dma((len(later),)),
            dma, dma,
            dma((E, D)), dma((D, E)),
            dma((D - 1, D, E)), dma((D - 1, D, E)),
            dma((q - 1, D, D, E)), dma((q - 1, D, D, E)),
        ],
        cost_estimate=pl.CostEstimate(flops=2 * 10**10, bytes_accessed=2**22, transcendentals=0),
        compiler_params=pltpu.CompilerParams(has_side_effects=True, collective_id=0),
    )(expert_ids.T, route_gates.T, grad_out, hidden)
    arrived = [lax.ppermute(part, "dp", swap) for part in parts]

    def run(base, others, out):
        spans = tuple(o.shape[1] for o in others)
        count = sum(spans) // tile
        slots = min(4, count)
        return pl.pallas_call(
            functools.partial(product, base, spans, tile, strip, slots),
            out_shape=jax.ShapeDtypeStruct((units, width), bf16),
            in_specs=[hbm] * (len(others) + 2 + len(out)),
            out_specs=hbm,
            scratch_shapes=[
                pltpu.VMEM((count, 2 * rows, tile), bf16),
                pltpu.VMEM((depth, width), bf16),
                pltpu.VMEM((slots, tile, width), bf16),
                dma((count, 2)), dma((width // strip,)), dma((slots,)),
            ],
            input_output_aliases={len(others) + 2: 0} if out else {},
            cost_estimate=pl.CostEstimate(
                flops=2 * depth * width * count * tile,
                bytes_accessed=2 * width * count * tile,
                transcendentals=0,
            ),
        )(hidden, *others, g, *out)

    out = run(0, (first, other), ())
    for (at, _), part in zip(later, arrived):
        out = run(at, (part,), (out,))
    return out[None]


def solution(mesh):
    in_specs = (
        P(("dp", "expert"), "tensor"),
        P(("dp", "expert"), None),
        P(("dp", "expert"), None),
        P("expert", "dp", "tensor"),
    )
    out_specs = P("expert", "tensor", "dp")
    return jax.shard_map(local, mesh=mesh, in_specs=in_specs, out_specs=out_specs, check_vma=False)
```

```python
import functools

import jax
import jax.numpy as jnp
from jax import lax
from jax.experimental import pallas as pl
from jax.experimental.pallas import tpu as pltpu
from jax.sharding import PartitionSpec as P


TOP = 2
CAP = 32
MESH = pl.DeviceIdType.MESH
TN = (((0,), (0,)), ((), ()))
EARLY, INSIDE, LATER = 2, 9, (4, 3)


def slot_table(expert_ids, route_gates, expert_count):
    routes = expert_ids.reshape(-1)
    weights = route_gates.reshape(-1)
    onehot = (routes[:, None] == jnp.arange(expert_count, dtype=jnp.int32)[None, :]).astype(
        jnp.int32
    )
    before = jnp.cumsum(onehot, axis=0) - onehot
    rank = jnp.sum(before * onehot, axis=1)
    target = jnp.where(rank < CAP, routes * CAP + rank, -1)
    match = jnp.arange(expert_count * CAP, dtype=jnp.int32)[:, None] == target[None, :]
    chosen = match.reshape(expert_count * CAP, -1, TOP).any(axis=2)
    slot_gate = jnp.sum(
        jnp.where(match, weights[None, :], jnp.zeros_like(weights)[None, :]), axis=1
    )
    return (chosen.astype(jnp.bfloat16), slot_gate)


def plain(grad_out, expert_ids, route_gates, saved_hidden):
    data_count = lax.axis_size("dp")
    expert_count = lax.axis_size("expert")
    chosen, slot_gate = slot_table(expert_ids, route_gates, expert_count)
    width = grad_out.shape[1] * lax.axis_size("tensor")
    block_width = width // data_count
    complete = lax.all_gather(grad_out, "tensor", axis=1, tiled=True)
    parted = complete.reshape(complete.shape[0], data_count, block_width)
    picked = jnp.einsum("st,tdk->dsk", chosen, parted, preferred_element_type=jnp.float32)
    outgoing = (picked * slot_gate[None, :, None]).astype(jnp.bfloat16)
    outgoing = outgoing.reshape(data_count * expert_count, CAP, block_width)
    arrived = lax.all_to_all(outgoing, ("dp", "expert"), split_axis=0, concat_axis=0, tiled=True)
    received = arrived.reshape(-1, block_width)
    summed = lax.dot_general(
        lax.all_gather(saved_hidden[0], "dp", axis=0, tiled=True),
        received,
        TN,
        preferred_element_type=jnp.float32,
    )
    return summed.astype(jnp.bfloat16)[None]


def slot_rows(ids, gates, grad, experts):
    tokens = ids.shape[1]
    named, gate, rank = [], [], []
    for e in range(experts):
        first = (ids[0:1, :] == e).astype(jnp.float32)
        second = (ids[1:2, :] == e).astype(jnp.float32)
        named.append(jnp.broadcast_to(first + second, (CAP, tokens)))
        gate.append(jnp.broadcast_to(first * gates[0:1, :] + second * gates[1:2, :], (CAP, tokens)))
        rank.append(lax.broadcasted_iota(jnp.int32, (CAP, tokens), 0))
    named = jnp.concatenate(named, axis=0)
    gate = jnp.concatenate(gate, axis=0)
    rank = jnp.concatenate(rank, axis=0).astype(jnp.float32)
    row = lax.broadcasted_iota(jnp.int32, (tokens, tokens), 0)
    column = lax.broadcasted_iota(jnp.int32, (tokens, tokens), 1)
    earlier = jnp.where(row < column, 1.0, 0.0).astype(jnp.bfloat16)
    before = jnp.dot(named.astype(jnp.bfloat16), earlier, preferred_element_type=jnp.float32)
    chosen = jnp.where(before == rank, named, 0.0)
    slot_gate = jnp.sum(chosen * gate, axis=1, keepdims=True)
    picked = jnp.dot(chosen.astype(jnp.bfloat16), grad, preferred_element_type=jnp.float32)
    return (picked * slot_gate).astype(jnp.bfloat16)


def exchange(
    D, E, T, lo, hi, later, ids_ref, gates_ref, grad_ref, hidden_ref, g_ref, other_ref, *rest
):
    parts = rest[:len(later)]
    (slots, p_in, h_send, h_recv, s1, r1, s2, r2, s3, r3) = rest[len(later):]
    d, e, t = lax.axis_index("dp"), lax.axis_index("expert"), lax.axis_index("tensor")
    q = T // D
    x, c = t // q, t % q
    cols = grad_ref.shape[1]
    W = cols // D

    def hidden_copy():
        return pltpu.make_async_remote_copy(
            src_ref=hidden_ref.at[:, pl.ds(lo, hi - lo)],
            dst_ref=other_ref,
            send_sem=h_send,
            recv_sem=h_recv,
            device_id=((d + 1) % D, e, t),
            device_id_type=MESH,
        )

    def stage(i):
        at, size = later[i]
        return pltpu.make_async_copy(hidden_ref.at[:, pl.ds(at, size)], parts[i], p_in.at[i])

    barrier = pltpu.get_barrier_semaphore()

    def greet(to):
        pl.semaphore_signal(barrier, inc=1, device_id=to, device_id_type=MESH)

    for n in range(1, D):
        greet(((d + n) % D, e, t))
        greet((d, e, ((x + n) % D) * q + c))
    for p in range(1, q):
        greet((d, e, x * q + (c + p) % q))
    for n in range(D):
        for j in range(E):
            to = ((x + n) % D, (e + j) % E, d * q + c)
            if n == 0 and j == 0:
                pl.when(x != d)(functools.partial(greet, to))
            else:
                greet(to)
    for i in range(len(later)):
        stage(i).start()
    slots[...] = slot_rows(ids_ref[...], gates_ref[...], grad_ref[...], E)
    pl.semaphore_wait(barrier, 2 * (D - 1) + q - 1 + D * E - jnp.where(x == d, 1, 0))

    def place(r, source, x_at, c_at):
        return g_ref.at[
            pl.ds(pl.multiple_of(r * (E * CAP) + source * CAP, CAP), CAP),
            pl.ds(pl.multiple_of(c_at * cols + x_at * W, 128), W),
        ]

    def first(j, m):
        e2, x2 = (e + j) % E, (x + m) % D
        r = (d - x + D) % D
        src = slots.at[
            pl.ds(pl.multiple_of(e2 * CAP, CAP), CAP), pl.ds(pl.multiple_of(x2 * W, 128), W)
        ]
        return src, place(r, e, x2, c), r1.at[r, (E - j) % E], (x, e2, x2 * q + c)

    def first_remote(j, m):
        src, dst, sem, to = first(j, m)
        return pltpu.make_async_remote_copy(
            src_ref=src, dst_ref=dst, send_sem=s1.at[j, m], recv_sem=sem,
            device_id=to, device_id_type=MESH,
        )

    def first_local():
        src = slots.at[
            pl.ds(pl.multiple_of(e * CAP, CAP), CAP), pl.ds(pl.multiple_of(x * W, 128), W)
        ]
        return pltpu.make_async_copy(src, place(0, e, x, c), r1.at[0, 0])

    order = sorted(range(E), key=lambda j: -min(j, E - j))
    for j in order:
        for m in range(D):
            if j == 0 and m == 0:
                pl.when(x == d)(lambda: first_local().start())
                pl.when(x != d)(lambda: first_remote(0, 0).start())
            else:
                first_remote(j, m).start()

    hidden_copy().start()

    def along(n, r, k):
        here = place(r, (e + k) % E, x, c)
        return pltpu.make_async_remote_copy(
            src_ref=here, dst_ref=here, send_sem=s2.at[n - 1, r, k], recv_sem=r2.at[D - n - 1, r, k],
            device_id=(d, e, ((x + n) % D) * q + c), device_id_type=MESH,
        )

    def along_arrived(n, r, k):
        here = place(r, (e + k) % E, (x + n) % D, c)
        return pltpu.make_async_remote_copy(
            src_ref=here, dst_ref=here, send_sem=s2.at[n - 1, r, k], recv_sem=r2.at[n - 1, r, k],
            device_id=(d, e, ((x + n) % D) * q + c), device_id_type=MESH,
        )

    def across(p, n, r, k):
        here = place(r, (e + k) % E, (x + n) % D, c)
        return pltpu.make_async_remote_copy(
            src_ref=here, dst_ref=here, send_sem=s3.at[p - 1, n, r, k],
            recv_sem=r3.at[q - p - 1, n, r, k],
            device_id=(d, e, x * q + (c + p) % q), device_id_type=MESH,
        )

    def across_arrived(p, n, r, k):
        here = place(r, (e + k) % E, (x + n) % D, (c + p) % q)
        return pltpu.make_async_remote_copy(
            src_ref=here, dst_ref=here, send_sem=s3.at[p - 1, n, r, k],
            recv_sem=r3.at[p - 1, n, r, k],
            device_id=(d, e, x * q + (c + p) % q), device_id_type=MESH,
        )

    def first_arrived(r, k):
        here = place(r, (e + k) % E, x, c)
        return pltpu.make_async_remote_copy(
            src_ref=here, dst_ref=here, send_sem=s1.at[0, 0], recv_sem=r1.at[r, k],
            device_id=((d + r) % D, (e + k) % E, d * q + c), device_id_type=MESH,
        )

    blocks = [(r, k) for k in reversed(order) for r in range(D)]
    for r, k in blocks:
        if r == 0 and k == 0:
            pl.when(x == d)(lambda: first_local().wait())
            pl.when(x != d)(lambda: first_arrived(0, 0).wait_recv())
        else:
            first_arrived(r, k).wait_recv()
        for n in range(1, D):
            along(n, r, k).start()
        for p in range(1, q):
            across(p, 0, r, k).start()
    for r, k in blocks:
        for n in range(1, D):
            along_arrived(n, r, k).wait_recv()
            for p in range(1, q):
                across(p, n, r, k).start()
    for r, k in blocks:
        for p in range(1, q):
            for n in range(D):
                across_arrived(p, n, r, k).wait_recv()
    for j in order:
        for m in range(D):
            if j == 0 and m == 0:
                pl.when(x != d)(lambda: first_remote(0, 0).wait_send())
            else:
                first_remote(j, m).wait_send()
    for r, k in blocks:
        for n in range(1, D):
            along(n, r, k).wait_send()
        for p in range(1, q):
            for n in range(D):
                across(p, n, r, k).wait_send()
    for i in range(len(later)):
        stage(i).wait()
    hidden_copy().wait()


def product(base, spans, tile, strip, slots, own_ref, *refs):
    others = refs[:len(spans)]
    g_ref = refs[len(spans)]
    o_ref, ob, os = refs[-3:]
    width = g_ref.shape[1]
    tiles = [(o, at) for o, size in zip(others, spans) for at in range(0, size, tile)]
    count = len(tiles)
    depth = min(slots, count)

    def leave(k):
        return pltpu.make_async_copy(
            ob.at[k % depth], o_ref.at[pl.ds(base + k * tile, tile), :], os.at[k % depth]
        )

    for k, (other, at) in enumerate(tiles):
        if k >= depth:
            leave(k - depth).wait()
        mine = own_ref[:, base + k * tile:base + (k + 1) * tile]
        hidden = jnp.concatenate([mine, other[:, at:at + tile]], axis=0)
        for lo in range(0, width, strip):
            ob[k % depth, :, lo:lo + strip] = lax.dot_general(
                hidden, g_ref[:, lo:lo + strip], TN, preferred_element_type=jnp.float32
            ).astype(ob.dtype)
        leave(k).start()
    for k in range(count - depth, count):
        leave(k).wait()


def local(grad_out, expert_ids, route_gates, saved_hidden):
    D, E, T = lax.axis_size("dp"), lax.axis_size("expert"), lax.axis_size("tensor")
    tokens, cols = grad_out.shape
    rows, units = saved_hidden.shape[1:]
    depth = D * E * CAP
    width = cols * T // D
    tile, strip = 256, 1024
    if (
        D != 2 or T % D or cols % (128 * D) or units % (16 * tile) or width % strip
        or rows != E * CAP or tokens % 128
    ):
        return plain(grad_out, expert_ids, route_gates, saved_hidden)
    q = T // D
    hidden = saved_hidden[0]
    share = units // 16
    ahead, stop = EARLY * share, INSIDE * share
    later, at = [], stop
    for part in LATER:
        later.append((at, part * share))
        at += part * share
    later = tuple(later)
    vmem = pl.BlockSpec(memory_space=pltpu.VMEM)
    hbm = pl.BlockSpec(memory_space=pltpu.HBM)
    dma = pltpu.SemaphoreType.DMA
    bf16 = jnp.bfloat16
    swap = [(0, 1), (1, 0)]
    first = lax.ppermute(hidden[:, :ahead], "dp", swap)
    g, other, *parts = pl.pallas_call(
        functools.partial(exchange, D, E, T, ahead, stop, later),
        out_shape=(
            jax.ShapeDtypeStruct((depth, width), bf16),
            jax.ShapeDtypeStruct((rows, stop - ahead), bf16),
            *(jax.ShapeDtypeStruct((rows, size), bf16) for _, size in later),
        ),
        in_specs=[vmem, vmem, vmem, hbm],
        out_specs=(vmem, vmem, *(vmem for _ in later)),
        scratch_shapes=[
            pltpu.VMEM((E * CAP, cols), bf16),
            dma((len(later),)),
            dma, dma,
            dma((E, D)), dma((D, E)),
            dma((D - 1, D, E)), dma((D - 1, D, E)),
            dma((q - 1, D, D, E)), dma((q - 1, D, D, E)),
        ],
        cost_estimate=pl.CostEstimate(flops=2 * 10**10, bytes_accessed=2**22, transcendentals=0),
        compiler_params=pltpu.CompilerParams(has_side_effects=True, collective_id=0, vmem_limit_bytes=16 * 2**20),
    )(expert_ids.T, route_gates.T, grad_out, hidden)
    arrived = []
    for part in parts:
        arrived.append(lax.ppermute(part, "dp", swap))

    def run(base, others, out):
        spans = tuple(o.shape[1] for o in others)
        count = sum(spans) // tile
        slots = min(6, count)
        return pl.pallas_call(
            functools.partial(product, base, spans, tile, strip, slots),
            out_shape=jax.ShapeDtypeStruct((units, width), bf16),
            in_specs=[vmem, *(vmem for _ in others), vmem, *(hbm for _ in out)],
            out_specs=hbm,
            scratch_shapes=[
                pltpu.VMEM((slots, tile, width), bf16),
                dma((slots,)),
            ],
            compiler_params=pltpu.CompilerParams(vmem_limit_bytes=24 * 2**20),
            input_output_aliases={len(others) + 2: 0} if out else {},
            cost_estimate=pl.CostEstimate(
                flops=2 * depth * width * count * tile,
                bytes_accessed=2 * width * count * tile,
                transcendentals=0,
            ),
        )(hidden, *others, g, *out)

    out = run(0, (first, other), ())
    for (at, _), part in zip(later, arrived):
        out = run(at, (part,), (out,))
    return out[None]


def solution(mesh):
    in_specs = (
        P(("dp", "expert"), "tensor"),
        P(("dp", "expert"), None),
        P(("dp", "expert"), None),
        P("expert", "dp", "tensor"),
    )
    out_specs = P("expert", "tensor", "dp")
    return jax.shard_map(local, mesh=mesh, in_specs=in_specs, out_specs=out_specs, check_vma=False)
```

```python
import functools

import jax
import jax.numpy as jnp
from jax import lax
from jax.experimental import pallas as pl
from jax.experimental.pallas import tpu as pltpu
from jax.sharding import PartitionSpec as P


TOP = 2
CAP = 32
MESH = pl.DeviceIdType.MESH
TN = (((0,), (0,)), ((), ()))
EARLY, INSIDE, LATER = 0, 9, (4, 3)


def slot_table(expert_ids, route_gates, expert_count):
    routes = expert_ids.reshape(-1)
    weights = route_gates.reshape(-1)
    onehot = (routes[:, None] == jnp.arange(expert_count, dtype=jnp.int32)[None, :]).astype(
        jnp.int32
    )
    before = jnp.cumsum(onehot, axis=0) - onehot
    rank = jnp.sum(before * onehot, axis=1)
    target = jnp.where(rank < CAP, routes * CAP + rank, -1)
    match = jnp.arange(expert_count * CAP, dtype=jnp.int32)[:, None] == target[None, :]
    chosen = match.reshape(expert_count * CAP, -1, TOP).any(axis=2)
    slot_gate = jnp.sum(
        jnp.where(match, weights[None, :], jnp.zeros_like(weights)[None, :]), axis=1
    )
    return (chosen.astype(jnp.bfloat16), slot_gate)


def plain(grad_out, expert_ids, route_gates, saved_hidden):
    data_count = lax.axis_size("dp")
    expert_count = lax.axis_size("expert")
    chosen, slot_gate = slot_table(expert_ids, route_gates, expert_count)
    width = grad_out.shape[1] * lax.axis_size("tensor")
    block_width = width // data_count
    complete = lax.all_gather(grad_out, "tensor", axis=1, tiled=True)
    parted = complete.reshape(complete.shape[0], data_count, block_width)
    picked = jnp.einsum("st,tdk->dsk", chosen, parted, preferred_element_type=jnp.float32)
    outgoing = (picked * slot_gate[None, :, None]).astype(jnp.bfloat16)
    outgoing = outgoing.reshape(data_count * expert_count, CAP, block_width)
    arrived = lax.all_to_all(outgoing, ("dp", "expert"), split_axis=0, concat_axis=0, tiled=True)
    received = arrived.reshape(-1, block_width)
    summed = lax.dot_general(
        lax.all_gather(saved_hidden[0], "dp", axis=0, tiled=True),
        received,
        TN,
        preferred_element_type=jnp.float32,
    )
    return summed.astype(jnp.bfloat16)[None]


def slot_rows(ids, gates, grad, experts):
    tokens = ids.shape[1]
    named, gate, rank = [], [], []
    for e in range(experts):
        first = (ids[0:1, :] == e).astype(jnp.float32)
        second = (ids[1:2, :] == e).astype(jnp.float32)
        named.append(jnp.broadcast_to(first + second, (CAP, tokens)))
        gate.append(jnp.broadcast_to(first * gates[0:1, :] + second * gates[1:2, :], (CAP, tokens)))
        rank.append(lax.broadcasted_iota(jnp.int32, (CAP, tokens), 0))
    named = jnp.concatenate(named, axis=0)
    gate = jnp.concatenate(gate, axis=0)
    rank = jnp.concatenate(rank, axis=0).astype(jnp.float32)
    row = lax.broadcasted_iota(jnp.int32, (tokens, tokens), 0)
    column = lax.broadcasted_iota(jnp.int32, (tokens, tokens), 1)
    earlier = jnp.where(row < column, 1.0, 0.0).astype(jnp.bfloat16)
    before = jnp.dot(named.astype(jnp.bfloat16), earlier, preferred_element_type=jnp.float32)
    chosen = jnp.where(before == rank, named, 0.0)
    slot_gate = jnp.sum(chosen * gate, axis=1, keepdims=True)
    picked = jnp.dot(chosen.astype(jnp.bfloat16), grad, preferred_element_type=jnp.float32)
    return (picked * slot_gate).astype(jnp.bfloat16)


def flip(e, j):
    return sum(((e // b + j // b) % 2) * b for b in (1, 2, 4, 8, 16))


def exchange(
    D, E, T, lo, hi, later, ids_hbm, gates_hbm, grad_hbm, hidden_ref, g_ref, other_ref, *rest
):
    parts = rest[:len(later)]
    (ids_ref, gates_ref, grad_ref, loads, slots, p_in, h_send, h_recv, s1, r1, s2, r2, s3, r3) = rest[len(later):]
    d, e, t = lax.axis_index("dp"), lax.axis_index("expert"), lax.axis_index("tensor")
    q = T // D
    x, c = t // q, t % q
    cols = grad_ref.shape[1]
    W = cols // D

    def hidden_copy():
        return pltpu.make_async_remote_copy(
            src_ref=hidden_ref.at[:, pl.ds(lo, hi - lo)],
            dst_ref=other_ref,
            send_sem=h_send,
            recv_sem=h_recv,
            device_id=((d + 1) % D, e, t),
            device_id_type=MESH,
        )

    def stage(i):
        at, size = later[i]
        return pltpu.make_async_copy(hidden_ref.at[:, pl.ds(at, size)], parts[i], p_in.at[i])

    inputs = [
        pltpu.make_async_copy(source, target, loads.at[i])
        for i, (source, target) in enumerate(
            ((ids_hbm, ids_ref), (gates_hbm, gates_ref), (grad_hbm, grad_ref))
        )
    ]
    for copy in inputs:
        copy.start()
    barrier = pltpu.get_barrier_semaphore()

    def greet(to):
        pl.semaphore_signal(barrier, inc=1, device_id=to, device_id_type=MESH)

    for n in range(1, D):
        greet(((d + n) % D, e, t))
        greet((d, e, ((x + n) % D) * q + c))
    for p in range(1, q):
        greet((d, e, x * q + (c + p) % q))
    for n in range(D):
        for j in range(E):
            to = ((x + n) % D, (e + j) % E, d * q + c)
            if n == 0 and j == 0:
                pl.when(x != d)(functools.partial(greet, to))
            else:
                greet(to)
    for i in range(len(later)):
        stage(i).start()
    for copy in inputs:
        copy.wait()
    slots[...] = slot_rows(ids_ref[...], gates_ref[...], grad_ref[...], E)
    pl.semaphore_wait(barrier, 2 * (D - 1) + q - 1 + D * E - jnp.where(x == d, 1, 0))

    def place(r, source, x_at, c_at):
        return g_ref.at[
            pl.ds(pl.multiple_of(r * (E * CAP) + source * CAP, CAP), CAP),
            pl.ds(pl.multiple_of(c_at * cols + x_at * W, 128), W),
        ]

    def first(j, m):
        e2, x2 = flip(e, j), (x + m) % D
        r = (d - x + D) % D
        src = slots.at[
            pl.ds(pl.multiple_of(e2 * CAP, CAP), CAP), pl.ds(pl.multiple_of(x2 * W, 128), W)
        ]
        return src, place(r, e, x2, c), r1.at[r, j], (x, e2, x2 * q + c)

    def first_remote(j, m):
        src, dst, sem, to = first(j, m)
        return pltpu.make_async_remote_copy(
            src_ref=src, dst_ref=dst, send_sem=s1.at[j, m], recv_sem=sem,
            device_id=to, device_id_type=MESH,
        )

    def first_local():
        src = slots.at[
            pl.ds(pl.multiple_of(e * CAP, CAP), CAP), pl.ds(pl.multiple_of(x * W, 128), W)
        ]
        return pltpu.make_async_copy(src, place(0, e, x, c), r1.at[0, 0])

    order = [0, 1, 2, 3]
    for j in order:
        for m in range(D):
            if j == 0 and m == 0:
                pl.when(x == d)(lambda: first_local().start())
                pl.when(x != d)(lambda: first_remote(0, 0).start())
            else:
                first_remote(j, m).start()

    hidden_copy().start()

    def along(n, r, k):
        here = place(r, flip(e, k), x, c)
        return pltpu.make_async_remote_copy(
            src_ref=here, dst_ref=here, send_sem=s2.at[n - 1, r, k], recv_sem=r2.at[D - n - 1, r, k],
            device_id=(d, e, ((x + n) % D) * q + c), device_id_type=MESH,
        )

    def along_arrived(n, r, k):
        here = place(r, flip(e, k), (x + n) % D, c)
        return pltpu.make_async_remote_copy(
            src_ref=here, dst_ref=here, send_sem=s2.at[n - 1, r, k], recv_sem=r2.at[n - 1, r, k],
            device_id=(d, e, ((x + n) % D) * q + c), device_id_type=MESH,
        )

    def across(p, n, r, k):
        here = place(r, flip(e, k), (x + n) % D, c)
        return pltpu.make_async_remote_copy(
            src_ref=here, dst_ref=here, send_sem=s3.at[p - 1, n, r, k],
            recv_sem=r3.at[q - p - 1, n, r, k],
            device_id=(d, e, x * q + (c + p) % q), device_id_type=MESH,
        )

    def across_arrived(p, n, r, k):
        here = place(r, flip(e, k), (x + n) % D, (c + p) % q)
        return pltpu.make_async_remote_copy(
            src_ref=here, dst_ref=here, send_sem=s3.at[p - 1, n, r, k],
            recv_sem=r3.at[p - 1, n, r, k],
            device_id=(d, e, x * q + (c + p) % q), device_id_type=MESH,
        )

    def first_arrived(r, k):
        here = place(r, flip(e, k), x, c)
        return pltpu.make_async_remote_copy(
            src_ref=here, dst_ref=here, send_sem=s1.at[0, 0], recv_sem=r1.at[r, k],
            device_id=((d + r) % D, flip(e, k), d * q + c), device_id_type=MESH,
        )

    blocks = [(r, k) for k in range(E) for r in range(D)]
    for r, k in blocks:
        if r == 0 and k == 0:
            pl.when(x == d)(lambda: first_local().wait())
            pl.when(x != d)(lambda: first_arrived(0, 0).wait_recv())
        else:
            first_arrived(r, k).wait_recv()
        for n in range(1, D):
            along(n, r, k).start()
        for p in range(1, q):
            across(p, 0, r, k).start()
    for r, k in blocks:
        for n in range(1, D):
            along_arrived(n, r, k).wait_recv()
            for p in range(1, q):
                across(p, n, r, k).start()
    for r, k in blocks:
        for p in range(1, q):
            for n in range(D):
                across_arrived(p, n, r, k).wait_recv()
    for j in order:
        for m in range(D):
            if j == 0 and m == 0:
                pl.when(x != d)(lambda: first_remote(0, 0).wait_send())
            else:
                first_remote(j, m).wait_send()
    for r, k in blocks:
        for n in range(1, D):
            along(n, r, k).wait_send()
        for p in range(1, q):
            for n in range(D):
                across(p, n, r, k).wait_send()
    for i in range(len(later)):
        stage(i).wait()
    hidden_copy().wait()


def product(base, spans, tile, strip, slots, own_ref, *refs):
    others = refs[:len(spans)]
    g_ref = refs[len(spans)]
    o_ref, ob, os = refs[-3:]
    width = g_ref.shape[1]
    tiles = [(o, at) for o, size in zip(others, spans) for at in range(0, size, tile)]
    count = len(tiles)
    depth = min(slots, count)

    starts = range(0, width, strip)

    def leave(k, i):
        return pltpu.make_async_copy(
            ob.at[k % depth, :, pl.ds(starts[i], strip)],
            o_ref.at[pl.ds(base + k * tile, tile), pl.ds(starts[i], strip)],
            os.at[k % depth, i],
        )

    for k, (other, at) in enumerate(tiles):
        mine = own_ref[:, base + k * tile:base + (k + 1) * tile]
        hidden = jnp.concatenate([mine, other[:, at:at + tile]], axis=0)
        for i, lo in enumerate(starts):
            if k >= depth:
                leave(k - depth, i).wait()
            ob[k % depth, :, lo:lo + strip] = lax.dot_general(
                hidden, g_ref[:, lo:lo + strip], TN, preferred_element_type=jnp.float32
            ).astype(ob.dtype)
            leave(k, i).start()
    for k in range(count - depth, count):
        for i in range(len(starts)):
            leave(k, i).wait()


def local(grad_out, expert_ids, route_gates, saved_hidden):
    D, E, T = lax.axis_size("dp"), lax.axis_size("expert"), lax.axis_size("tensor")
    tokens, cols = grad_out.shape
    rows, units = saved_hidden.shape[1:]
    depth = D * E * CAP
    width = cols * T // D
    tile, strip = 256, 1024
    if (
        D != 2 or E & (E - 1) or E > 32 or T % D or cols % (128 * D) or units % (16 * tile) or width % strip
        or rows != E * CAP or tokens % 128
    ):
        return plain(grad_out, expert_ids, route_gates, saved_hidden)
    q = T // D
    hidden = saved_hidden[0]
    share = units // 16
    ahead, stop = EARLY * share, INSIDE * share
    later, at = [], stop
    for part in LATER:
        later.append((at, part * share))
        at += part * share
    later = tuple(later)
    vmem = pl.BlockSpec(memory_space=pltpu.VMEM)
    hbm = pl.BlockSpec(memory_space=pltpu.HBM)
    dma = pltpu.SemaphoreType.DMA
    bf16 = jnp.bfloat16
    swap = [(0, 1), (1, 0)]
    g, other, *parts = pl.pallas_call(
        functools.partial(exchange, D, E, T, ahead, stop, later),
        out_shape=(
            pltpu.VMEM((depth, width), bf16),
            pltpu.VMEM((rows, stop - ahead), bf16),
            *(pltpu.VMEM((rows, size), bf16) for _, size in later),
        ),
        in_specs=[hbm] * 4,
        out_specs=(vmem, vmem, *(vmem for _ in later)),
        scratch_shapes=[
            pltpu.VMEM((TOP, tokens), jnp.int32),
            pltpu.VMEM((TOP, tokens), jnp.float32),
            pltpu.VMEM((tokens, cols), bf16),
            dma((3,)),
            pltpu.VMEM((E * CAP, cols), bf16),
            dma((len(later),)),
            dma, dma,
            dma((E, D)), dma((D, E)),
            dma((D - 1, D, E)), dma((D - 1, D, E)),
            dma((q - 1, D, D, E)), dma((q - 1, D, D, E)),
        ],
        cost_estimate=pl.CostEstimate(flops=2 * 10**10, bytes_accessed=2**22, transcendentals=0),
        compiler_params=pltpu.CompilerParams(has_side_effects=True, collective_id=0, vmem_limit_bytes=16777216),
    )(*(
        pltpu.with_memory_space_constraint(a, pltpu.HBM)
        for a in (expert_ids.T, route_gates.T, grad_out, hidden)
    ))
    arrived = []
    for part in parts:
        arrived.append(lax.ppermute(part, "dp", swap))

    def run(base, others, out):
        spans = tuple(o.shape[1] for o in others)
        count = sum(spans) // tile
        slots = min(6, count)
        return pl.pallas_call(
            functools.partial(product, base, spans, tile, strip, slots),
            out_shape=jax.ShapeDtypeStruct((units, width), bf16),
            in_specs=[vmem, *(vmem for _ in others), vmem, *(hbm for _ in out)],
            out_specs=hbm,
            scratch_shapes=[
                pltpu.VMEM((slots, tile, width), bf16),
                dma((slots, width // strip)),
            ],
            compiler_params=pltpu.CompilerParams(vmem_limit_bytes=24 * 2**20),
            input_output_aliases={len(others) + 2: 0} if out else {},
            cost_estimate=pl.CostEstimate(
                flops=2 * depth * width * count * tile,
                bytes_accessed=2 * width * count * tile,
                transcendentals=0,
            ),
        )(hidden, *others, g, *out)

    out = run(0, (other,), ())
    for (at, _), part in zip(later, arrived):
        out = run(at, (part,), (out,))
    return out[None]


def solution(mesh):
    in_specs = (
        P(("dp", "expert"), "tensor"),
        P(("dp", "expert"), None),
        P(("dp", "expert"), None),
        P("expert", "dp", "tensor"),
    )
    out_specs = P("expert", "tensor", "dp")
    return jax.shard_map(local, mesh=mesh, in_specs=in_specs, out_specs=out_specs, check_vma=False)
```

```python
import functools

import jax
import jax.numpy as jnp
from jax import lax
from jax.experimental import pallas as pl
from jax.experimental.pallas import tpu as pltpu
from jax.sharding import PartitionSpec as P


TOP = 2
CAP = 32
MESH = pl.DeviceIdType.MESH
TN = (((0,), (0,)), ((), ()))
EARLY, INSIDE, LATER = 4, 11, (5,)


def slot_table(expert_ids, route_gates, expert_count):
    routes = expert_ids.reshape(-1)
    weights = route_gates.reshape(-1)
    onehot = (routes[:, None] == jnp.arange(expert_count, dtype=jnp.int32)[None, :]).astype(
        jnp.int32
    )
    before = jnp.cumsum(onehot, axis=0) - onehot
    rank = jnp.sum(before * onehot, axis=1)
    target = jnp.where(rank < CAP, routes * CAP + rank, -1)
    match = jnp.arange(expert_count * CAP, dtype=jnp.int32)[:, None] == target[None, :]
    chosen = match.reshape(expert_count * CAP, -1, TOP).any(axis=2)
    slot_gate = jnp.sum(
        jnp.where(match, weights[None, :], jnp.zeros_like(weights)[None, :]), axis=1
    )
    return (chosen.astype(jnp.bfloat16), slot_gate)


def plain(grad_out, expert_ids, route_gates, saved_hidden):
    data_count = lax.axis_size("dp")
    expert_count = lax.axis_size("expert")
    chosen, slot_gate = slot_table(expert_ids, route_gates, expert_count)
    width = grad_out.shape[1] * lax.axis_size("tensor")
    block_width = width // data_count
    complete = lax.all_gather(grad_out, "tensor", axis=1, tiled=True)
    parted = complete.reshape(complete.shape[0], data_count, block_width)
    picked = jnp.einsum("st,tdk->dsk", chosen, parted, preferred_element_type=jnp.float32)
    outgoing = (picked * slot_gate[None, :, None]).astype(jnp.bfloat16)
    outgoing = outgoing.reshape(data_count * expert_count, CAP, block_width)
    arrived = lax.all_to_all(outgoing, ("dp", "expert"), split_axis=0, concat_axis=0, tiled=True)
    received = arrived.reshape(-1, block_width)
    summed = lax.dot_general(
        lax.all_gather(saved_hidden[0], "dp", axis=0, tiled=True),
        received,
        TN,
        preferred_element_type=jnp.float32,
    )
    return summed.astype(jnp.bfloat16)[None]


def slot_rows(ids, gates, grad, experts):
    tokens = ids.shape[1]
    named, gate, rank = [], [], []
    for e in range(experts):
        first = (ids[0:1, :] == e).astype(jnp.float32)
        second = (ids[1:2, :] == e).astype(jnp.float32)
        named.append(jnp.broadcast_to(first + second, (CAP, tokens)))
        gate.append(jnp.broadcast_to(first * gates[0:1, :] + second * gates[1:2, :], (CAP, tokens)))
        rank.append(lax.broadcasted_iota(jnp.int32, (CAP, tokens), 0))
    named = jnp.concatenate(named, axis=0)
    gate = jnp.concatenate(gate, axis=0)
    rank = jnp.concatenate(rank, axis=0).astype(jnp.float32)
    row = lax.broadcasted_iota(jnp.int32, (tokens, tokens), 0)
    column = lax.broadcasted_iota(jnp.int32, (tokens, tokens), 1)
    earlier = jnp.where(row < column, 1.0, 0.0).astype(jnp.bfloat16)
    before = jnp.dot(named.astype(jnp.bfloat16), earlier, preferred_element_type=jnp.float32)
    chosen = jnp.where(before == rank, named, 0.0)
    slot_gate = jnp.sum(chosen * gate, axis=1, keepdims=True)
    picked = jnp.dot(chosen.astype(jnp.bfloat16), grad, preferred_element_type=jnp.float32)
    return (picked * slot_gate).astype(jnp.bfloat16)


def flip(e, j):
    return sum(((e // b + j // b) % 2) * b for b in (1, 2, 4, 8, 16))


def exchange(
    D, E, T, lo, hi, later, ids_hbm, gates_hbm, grad_hbm, hidden_ref, g_ref, other_ref, *rest
):
    parts = rest[:len(later)]
    (ids_ref, gates_ref, grad_ref, near, loads, slots, p_in, h_send, h_recv, s1, r1, s2, r2, s3, r3) = rest[len(later):]
    d, e, t = lax.axis_index("dp"), lax.axis_index("expert"), lax.axis_index("tensor")
    q = T // D
    x, c = t // q, t % q
    cols = grad_ref.shape[1]
    W = cols // D

    def hidden_copy():
        return pltpu.make_async_remote_copy(
            src_ref=near,
            dst_ref=other_ref,
            send_sem=h_send,
            recv_sem=h_recv,
            device_id=((d + 1) % D, e, t),
            device_id_type=MESH,
        )

    def stage(i):
        at, size = later[i]
        return pltpu.make_async_copy(hidden_ref.at[:, pl.ds(at, size)], parts[i], p_in.at[i])

    inputs = [
        pltpu.make_async_copy(source, target, loads.at[i])
        for i, (source, target) in enumerate(
            (
                (ids_hbm, ids_ref), (gates_hbm, gates_ref), (grad_hbm, grad_ref),
                (hidden_ref.at[:, pl.ds(lo, hi - lo)], near),
            )
        )
    ]
    for copy in inputs:
        copy.start()
    barrier = pltpu.get_barrier_semaphore()

    def greet(to):
        pl.semaphore_signal(barrier, inc=1, device_id=to, device_id_type=MESH)

    for n in range(1, D):
        greet(((d + n) % D, e, t))
        greet((d, e, ((x + n) % D) * q + c))
    for p in range(1, q):
        greet((d, e, x * q + (c + p) % q))
    for n in range(D):
        for j in range(E):
            to = ((x + n) % D, (e + j) % E, d * q + c)
            if n == 0 and j == 0:
                pl.when(x != d)(functools.partial(greet, to))
            else:
                greet(to)
    for i in range(len(later)):
        stage(i).start()
    for copy in inputs[:3]:
        copy.wait()
    slots[...] = slot_rows(ids_ref[...], gates_ref[...], grad_ref[...], E)
    pl.semaphore_wait(barrier, 2 * (D - 1) + q - 1 + D * E - jnp.where(x == d, 1, 0))

    def place(r, source, x_at, c_at):
        return g_ref.at[
            pl.ds(pl.multiple_of(r * (E * CAP) + source * CAP, CAP), CAP),
            pl.ds(pl.multiple_of(c_at * cols + x_at * W, 128), W),
        ]

    def first(j, m):
        e2, x2 = flip(e, j), (x + m) % D
        r = (d - x + D) % D
        src = slots.at[
            pl.ds(pl.multiple_of(e2 * CAP, CAP), CAP), pl.ds(pl.multiple_of(x2 * W, 128), W)
        ]
        return src, place(r, e, x2, c), r1.at[r, j], (x, e2, x2 * q + c)

    def first_remote(j, m):
        src, dst, sem, to = first(j, m)
        return pltpu.make_async_remote_copy(
            src_ref=src, dst_ref=dst, send_sem=s1.at[j, m], recv_sem=sem,
            device_id=to, device_id_type=MESH,
        )

    def first_local():
        src = slots.at[
            pl.ds(pl.multiple_of(e * CAP, CAP), CAP), pl.ds(pl.multiple_of(x * W, 128), W)
        ]
        return pltpu.make_async_copy(src, place(0, e, x, c), r1.at[0, 0])

    order = [0, 1, 2, 3]
    for j in order:
        for m in range(D):
            if j == 0 and m == 0:
                pl.when(x == d)(lambda: first_local().start())
                pl.when(x != d)(lambda: first_remote(0, 0).start())
            else:
                first_remote(j, m).start()

    inputs[3].wait()
    hidden_copy().start()

    def along(n, r, k):
        here = place(r, flip(e, k), x, c)
        return pltpu.make_async_remote_copy(
            src_ref=here, dst_ref=here, send_sem=s2.at[n - 1, r, k], recv_sem=r2.at[D - n - 1, r, k],
            device_id=(d, e, ((x + n) % D) * q + c), device_id_type=MESH,
        )

    def along_arrived(n, r, k):
        here = place(r, flip(e, k), (x + n) % D, c)
        return pltpu.make_async_remote_copy(
            src_ref=here, dst_ref=here, send_sem=s2.at[n - 1, r, k], recv_sem=r2.at[n - 1, r, k],
            device_id=(d, e, ((x + n) % D) * q + c), device_id_type=MESH,
        )

    def across(p, n, r, k):
        here = place(r, flip(e, k), (x + n) % D, c)
        return pltpu.make_async_remote_copy(
            src_ref=here, dst_ref=here, send_sem=s3.at[p - 1, n, r, k],
            recv_sem=r3.at[q - p - 1, n, r, k],
            device_id=(d, e, x * q + (c + p) % q), device_id_type=MESH,
        )

    def across_arrived(p, n, r, k):
        here = place(r, flip(e, k), (x + n) % D, (c + p) % q)
        return pltpu.make_async_remote_copy(
            src_ref=here, dst_ref=here, send_sem=s3.at[p - 1, n, r, k],
            recv_sem=r3.at[p - 1, n, r, k],
            device_id=(d, e, x * q + (c + p) % q), device_id_type=MESH,
        )

    def first_arrived(r, k):
        here = place(r, flip(e, k), x, c)
        return pltpu.make_async_remote_copy(
            src_ref=here, dst_ref=here, send_sem=s1.at[0, 0], recv_sem=r1.at[r, k],
            device_id=((d + r) % D, flip(e, k), d * q + c), device_id_type=MESH,
        )

    blocks = [(r, k) for k in range(E) for r in range(D)]
    for r, k in blocks:
        if r == 0 and k == 0:
            pl.when(x == d)(lambda: first_local().wait())
            pl.when(x != d)(lambda: first_arrived(0, 0).wait_recv())
        else:
            first_arrived(r, k).wait_recv()
        for n in range(1, D):
            along(n, r, k).start()
        for p in range(1, q):
            across(p, 0, r, k).start()
    for r, k in blocks:
        for n in range(1, D):
            along_arrived(n, r, k).wait_recv()
            for p in range(1, q):
                across(p, n, r, k).start()
    for r, k in blocks:
        for p in range(1, q):
            for n in range(D):
                across_arrived(p, n, r, k).wait_recv()
    for j in order:
        for m in range(D):
            if j == 0 and m == 0:
                pl.when(x != d)(lambda: first_remote(0, 0).wait_send())
            else:
                first_remote(j, m).wait_send()
    for r, k in blocks:
        for n in range(1, D):
            along(n, r, k).wait_send()
        for p in range(1, q):
            for n in range(D):
                across(p, n, r, k).wait_send()
    for i in range(len(later)):
        stage(i).wait()
    hidden_copy().wait()


def product(base, spans, tile, strip, own_ref, *refs):
    others = refs[:len(spans)]
    g_ref = refs[len(spans)]
    o_ref, ob, os = refs[-3:]
    width = g_ref.shape[1]
    tiles = [(o, at) for o, size in zip(others, spans) for at in range(0, size, tile)]
    count = len(tiles)

    starts = range(0, width, strip)
    fine = 0 if count < 6 else count - 1
    pieces = [(k, 0, width) for k in range(fine)]
    pieces += [(k, lo, strip) for k in range(fine, count) for lo in starts]

    def leave(i):
        k, lo, size = pieces[i]
        return pltpu.make_async_copy(
            ob.at[k, :, pl.ds(lo, size)],
            o_ref.at[pl.ds(base + k * tile, tile), pl.ds(lo, size)],
            os.at[i],
        )

    for k, (other, at) in enumerate(tiles):
        mine = own_ref[:, base + k * tile:base + (k + 1) * tile]
        hidden = jnp.concatenate([mine, other[:, at:at + tile]], axis=0)
        for i, lo in enumerate(starts):
            ob[k, :, lo:lo + strip] = lax.dot_general(
                hidden, g_ref[:, lo:lo + strip], TN, preferred_element_type=jnp.float32
            ).astype(ob.dtype)
            if k >= fine:
                leave(fine + (k - fine) * len(starts) + i).start()
        if k < fine:
            leave(k).start()
    for i in range(len(pieces)):
        leave(i).wait()


def local(grad_out, expert_ids, route_gates, saved_hidden):
    D, E, T = lax.axis_size("dp"), lax.axis_size("expert"), lax.axis_size("tensor")
    tokens, cols = grad_out.shape
    rows, units = saved_hidden.shape[1:]
    depth = D * E * CAP
    width = cols * T // D
    tile, strip = 256, 1024
    if (
        D != 2 or E & (E - 1) or E > 32 or T % D or cols % (128 * D) or units % (16 * tile) or width % strip
        or rows != E * CAP or tokens % 128
    ):
        return plain(grad_out, expert_ids, route_gates, saved_hidden)
    q = T // D
    hidden = saved_hidden[0]
    share = units // 16
    ahead, stop = EARLY * share, INSIDE * share
    later, at = [], stop
    for part in LATER:
        later.append((at, part * share))
        at += part * share
    later = tuple(later)
    vmem = pl.BlockSpec(memory_space=pltpu.VMEM)
    hbm = pl.BlockSpec(memory_space=pltpu.HBM)
    dma = pltpu.SemaphoreType.DMA
    bf16 = jnp.bfloat16
    swap = [(0, 1), (1, 0)]
    first = lax.ppermute(hidden[:, :ahead], "dp", swap)
    g, other, *parts = pl.pallas_call(
        functools.partial(exchange, D, E, T, ahead, stop, later),
        out_shape=(
            pltpu.VMEM((depth, width), bf16),
            pltpu.VMEM((rows, stop - ahead), bf16),
            *(pltpu.VMEM((rows, size), bf16) for _, size in later),
        ),
        in_specs=[hbm] * 4,
        out_specs=(vmem, vmem, *(vmem for _ in later)),
        scratch_shapes=[
            pltpu.VMEM((TOP, tokens), jnp.int32),
            pltpu.VMEM((TOP, tokens), jnp.float32),
            pltpu.VMEM((tokens, cols), bf16),
            pltpu.VMEM((rows, stop - ahead), bf16),
            dma((4,)),
            pltpu.VMEM((E * CAP, cols), bf16),
            dma((len(later),)),
            dma, dma,
            dma((E, D)), dma((D, E)),
            dma((D - 1, D, E)), dma((D - 1, D, E)),
            dma((q - 1, D, D, E)), dma((q - 1, D, D, E)),
        ],
        cost_estimate=pl.CostEstimate(flops=2 * 10**10, bytes_accessed=2**22, transcendentals=0),
        compiler_params=pltpu.CompilerParams(has_side_effects=True, collective_id=0, vmem_limit_bytes=16777216),
    )(*(
        pltpu.with_memory_space_constraint(a, pltpu.HBM)
        for a in (expert_ids.T, route_gates.T, grad_out, hidden)
    ))
    arrived = []
    for part in parts:
        arrived.append(lax.ppermute(part, "dp", swap))

    def run(base, others, out):
        spans = tuple(o.shape[1] for o in others)
        count = sum(spans) // tile
        return pl.pallas_call(
            functools.partial(product, base, spans, tile, strip),
            out_shape=jax.ShapeDtypeStruct((units, width), bf16),
            in_specs=[vmem, *(vmem for _ in others), vmem, *(hbm for _ in out)],
            out_specs=hbm,
            scratch_shapes=[
                pltpu.VMEM((count, tile, width), bf16),
                dma((count + 6 * width // strip,)),
            ],
            compiler_params=pltpu.CompilerParams(vmem_limit_bytes=30 * 2**20),
            input_output_aliases={len(others) + 2: 0} if out else {},
            cost_estimate=pl.CostEstimate(
                flops=2 * depth * width * count * tile,
                bytes_accessed=2 * width * count * tile,
                transcendentals=0,
            ),
        )(hidden, *others, g, *out)

    out = run(0, (first, other), ())
    for (at, _), part in zip(later, arrived):
        out = run(at, (part,), (out,))
    return out[None]


def solution(mesh):
    in_specs = (
        P(("dp", "expert"), "tensor"),
        P(("dp", "expert"), None),
        P(("dp", "expert"), None),
        P("expert", "dp", "tensor"),
    )
    out_specs = P("expert", "tensor", "dp")
    return jax.shard_map(local, mesh=mesh, in_specs=in_specs, out_specs=out_specs, check_vma=False)
```

```python
import functools

import jax
import jax.numpy as jnp
from jax import lax
from jax.experimental import pallas as pl
from jax.experimental.pallas import tpu as pltpu
from jax.sharding import PartitionSpec as P


TOP = 2
CAP = 32
MESH = pl.DeviceIdType.MESH
TN = (((0,), (0,)), ((), ()))
EARLY, INSIDE, LATER, READY = 4, 11, (3, 2), 2


def slot_table(expert_ids, route_gates, expert_count):
    routes = expert_ids.reshape(-1)
    weights = route_gates.reshape(-1)
    onehot = (routes[:, None] == jnp.arange(expert_count, dtype=jnp.int32)[None, :]).astype(
        jnp.int32
    )
    before = jnp.cumsum(onehot, axis=0) - onehot
    rank = jnp.sum(before * onehot, axis=1)
    target = jnp.where(rank < CAP, routes * CAP + rank, -1)
    match = jnp.arange(expert_count * CAP, dtype=jnp.int32)[:, None] == target[None, :]
    chosen = match.reshape(expert_count * CAP, -1, TOP).any(axis=2)
    slot_gate = jnp.sum(
        jnp.where(match, weights[None, :], jnp.zeros_like(weights)[None, :]), axis=1
    )
    return (chosen.astype(jnp.bfloat16), slot_gate)


def plain(grad_out, expert_ids, route_gates, saved_hidden):
    data_count = lax.axis_size("dp")
    expert_count = lax.axis_size("expert")
    chosen, slot_gate = slot_table(expert_ids, route_gates, expert_count)
    width = grad_out.shape[1] * lax.axis_size("tensor")
    block_width = width // data_count
    complete = lax.all_gather(grad_out, "tensor", axis=1, tiled=True)
    parted = complete.reshape(complete.shape[0], data_count, block_width)
    picked = jnp.einsum("st,tdk->dsk", chosen, parted, preferred_element_type=jnp.float32)
    outgoing = (picked * slot_gate[None, :, None]).astype(jnp.bfloat16)
    outgoing = outgoing.reshape(data_count * expert_count, CAP, block_width)
    arrived = lax.all_to_all(outgoing, ("dp", "expert"), split_axis=0, concat_axis=0, tiled=True)
    received = arrived.reshape(-1, block_width)
    summed = lax.dot_general(
        lax.all_gather(saved_hidden[0], "dp", axis=0, tiled=True),
        received,
        TN,
        preferred_element_type=jnp.float32,
    )
    return summed.astype(jnp.bfloat16)[None]


def slot_rows(ids, gates, grad, experts):
    tokens = ids.shape[1]
    named, gate, rank = [], [], []
    for e in range(experts):
        first = (ids[0:1, :] == e).astype(jnp.float32)
        second = (ids[1:2, :] == e).astype(jnp.float32)
        named.append(jnp.broadcast_to(first + second, (CAP, tokens)))
        gate.append(jnp.broadcast_to(first * gates[0:1, :] + second * gates[1:2, :], (CAP, tokens)))
        rank.append(lax.broadcasted_iota(jnp.int32, (CAP, tokens), 0))
    named = jnp.concatenate(named, axis=0)
    gate = jnp.concatenate(gate, axis=0)
    rank = jnp.concatenate(rank, axis=0).astype(jnp.float32)
    row = lax.broadcasted_iota(jnp.int32, (tokens, tokens), 0)
    column = lax.broadcasted_iota(jnp.int32, (tokens, tokens), 1)
    earlier = jnp.where(row < column, 1.0, 0.0).astype(jnp.bfloat16)
    before = jnp.dot(named.astype(jnp.bfloat16), earlier, preferred_element_type=jnp.float32)
    chosen = jnp.where(before == rank, named, 0.0)
    slot_gate = jnp.sum(chosen * gate, axis=1, keepdims=True)
    picked = jnp.dot(chosen.astype(jnp.bfloat16), grad, preferred_element_type=jnp.float32)
    return (picked * slot_gate).astype(jnp.bfloat16)


def flip(e, j):
    return sum(((e // b + j // b) % 2) * b for b in (1, 2, 4, 8, 16))


def multiply(mine, other, g_ref, out_ref, strip, after=lambda lo: None):
    hidden = jnp.concatenate([mine, other], axis=0)
    for lo in range(0, g_ref.shape[1], strip):
        out_ref[:, lo:lo + strip] = lax.dot_general(
            hidden, g_ref[:, lo:lo + strip], TN, preferred_element_type=jnp.float32
        ).astype(out_ref.dtype)
        after(lo)


def exchange(
    D, E, T, lo, hi, done, tile, strip, later, ids_hbm, gates_hbm, grad_hbm, hidden_ref, g_ref, other_ref, pre_ref,
    *rest
):
    parts = rest[:len(later)]
    (
        ids_ref, gates_ref, grad_ref, near, loads, slots, p_in, h_send, h_recv, s1, r1, s2, r2, s3, r3
    ) = rest[len(later):]
    d, e, t = lax.axis_index("dp"), lax.axis_index("expert"), lax.axis_index("tensor")
    q = T // D
    x, c = t // q, t % q
    cols = grad_ref.shape[1]
    W = cols // D

    cuts = (0, done, hi - lo)

    def hidden_copy(i):
        part = pl.ds(cuts[i], cuts[i + 1] - cuts[i])
        return pltpu.make_async_remote_copy(
            src_ref=near.at[:, part],
            dst_ref=other_ref.at[:, part],
            send_sem=h_send.at[i],
            recv_sem=h_recv.at[i],
            device_id=((d + 1) % D, e, t),
            device_id_type=MESH,
        )

    def stage(i):
        at, size = later[i]
        return pltpu.make_async_copy(hidden_ref.at[:, pl.ds(at, size)], parts[i], p_in.at[i])

    inputs = [
        pltpu.make_async_copy(source, target, loads.at[i])
        for i, (source, target) in enumerate(
            (
                (ids_hbm, ids_ref), (gates_hbm, gates_ref), (grad_hbm, grad_ref),
                (hidden_ref.at[:, pl.ds(lo, hi - lo)], near),
            )
        )
    ]
    for copy in inputs:
        copy.start()
    barrier = pltpu.get_barrier_semaphore()

    def greet(to):
        pl.semaphore_signal(barrier, inc=1, device_id=to, device_id_type=MESH)

    for n in range(1, D):
        greet(((d + n) % D, e, t))
        greet((d, e, ((x + n) % D) * q + c))
    for p in range(1, q):
        greet((d, e, x * q + (c + p) % q))
    for n in range(D):
        for j in range(E):
            to = ((x + n) % D, (e + j) % E, d * q + c)
            if n == 0 and j == 0:
                pl.when(x != d)(functools.partial(greet, to))
            else:
                greet(to)
    for i in range(len(later)):
        stage(i).start()
    for copy in inputs[:3]:
        copy.wait()
    slots[...] = slot_rows(ids_ref[...], gates_ref[...], grad_ref[...], E)
    pl.semaphore_wait(barrier, 2 * (D - 1) + q - 1 + D * E - jnp.where(x == d, 1, 0))

    def place(r, source, x_at, c_at):
        return g_ref.at[
            pl.ds(pl.multiple_of(r * (E * CAP) + source * CAP, CAP), CAP),
            pl.ds(pl.multiple_of(c_at * cols + x_at * W, 128), W),
        ]

    def first(j, m):
        e2, x2 = flip(e, j), (x + m) % D
        r = (d - x + D) % D
        src = slots.at[
            pl.ds(pl.multiple_of(e2 * CAP, CAP), CAP), pl.ds(pl.multiple_of(x2 * W, 128), W)
        ]
        return src, place(r, e, x2, c), r1.at[r, j], (x, e2, x2 * q + c)

    def first_remote(j, m):
        src, dst, sem, to = first(j, m)
        return pltpu.make_async_remote_copy(
            src_ref=src, dst_ref=dst, send_sem=s1.at[j, m], recv_sem=sem,
            device_id=to, device_id_type=MESH,
        )

    def first_local():
        src = slots.at[
            pl.ds(pl.multiple_of(e * CAP, CAP), CAP), pl.ds(pl.multiple_of(x * W, 128), W)
        ]
        return pltpu.make_async_copy(src, place(0, e, x, c), r1.at[0, 0])

    order = range(E)
    for j in order:
        for m in range(D):
            if j == 0 and m == 0:
                pl.when(x == d)(lambda: first_local().start())
                pl.when(x != d)(lambda: first_remote(0, 0).start())
            else:
                first_remote(j, m).start()

    inputs[3].wait()
    for i in range(2):
        hidden_copy(i).start()

    def along(n, r, k):
        here = place(r, flip(e, k), x, c)
        return pltpu.make_async_remote_copy(
            src_ref=here, dst_ref=here, send_sem=s2.at[n - 1, r, k], recv_sem=r2.at[D - n - 1, r, k],
            device_id=(d, e, ((x + n) % D) * q + c), device_id_type=MESH,
        )

    def along_arrived(n, r, k):
        here = place(r, flip(e, k), (x + n) % D, c)
        return pltpu.make_async_remote_copy(
            src_ref=here, dst_ref=here, send_sem=s2.at[n - 1, r, k], recv_sem=r2.at[n - 1, r, k],
            device_id=(d, e, ((x + n) % D) * q + c), device_id_type=MESH,
        )

    def across(p, n, r, k):
        here = place(r, flip(e, k), (x + n) % D, c)
        return pltpu.make_async_remote_copy(
            src_ref=here, dst_ref=here, send_sem=s3.at[p - 1, n, r, k],
            recv_sem=r3.at[q - p - 1, n, r, k],
            device_id=(d, e, x * q + (c + p) % q), device_id_type=MESH,
        )

    def across_arrived(p, n, r, k):
        here = place(r, flip(e, k), (x + n) % D, (c + p) % q)
        return pltpu.make_async_remote_copy(
            src_ref=here, dst_ref=here, send_sem=s3.at[p - 1, n, r, k],
            recv_sem=r3.at[p - 1, n, r, k],
            device_id=(d, e, x * q + (c + p) % q), device_id_type=MESH,
        )

    def first_arrived(r, k):
        here = place(r, flip(e, k), x, c)
        return pltpu.make_async_remote_copy(
            src_ref=here, dst_ref=here, send_sem=s1.at[0, 0], recv_sem=r1.at[r, k],
            device_id=((d + r) % D, flip(e, k), d * q + c), device_id_type=MESH,
        )

    blocks = [(r, k) for k in range(E) for r in range(D)]
    for r, k in blocks:
        if r == 0 and k == 0:
            pl.when(x == d)(lambda: first_local().wait())
            pl.when(x != d)(lambda: first_arrived(0, 0).wait_recv())
        else:
            first_arrived(r, k).wait_recv()
        for n in range(1, D):
            along(n, r, k).start()
        for p in range(1, q):
            across(p, 0, r, k).start()
    for r, k in blocks:
        for n in range(1, D):
            along_arrived(n, r, k).wait_recv()
            for p in range(1, q):
                across(p, n, r, k).start()
    for r, k in blocks:
        for p in range(1, q):
            for n in range(D):
                across_arrived(p, n, r, k).wait_recv()
    hidden_copy(0).wait_recv()
    for at in range(0, done, tile):
        multiply(near[:, at:at + tile], other_ref[:, at:at + tile], g_ref, pre_ref.at[pl.ds(at, tile)], strip)
    for j in order:
        for m in range(D):
            if j == 0 and m == 0:
                pl.when(x != d)(lambda: first_remote(0, 0).wait_send())
            else:
                first_remote(j, m).wait_send()
    for r, k in blocks:
        for n in range(1, D):
            along(n, r, k).wait_send()
        for p in range(1, q):
            for n in range(D):
                across(p, n, r, k).wait_send()
    for i in range(len(later)):
        stage(i).wait()
    hidden_copy(0).wait_send()
    hidden_copy(1).wait()


def product(base, tiles, ready, tile, strip, own_ref, *refs):
    o_ref, ob, os = refs[-3:]
    others = refs[:1 + max(i for _, i, _ in tiles)]
    g_ref, *whole = refs[len(others):-3]
    width = g_ref.shape[1]
    count = len(tiles)
    fine = 0 if count < 6 else count - 1
    sent = []

    def send(source, row, lo, size):
        copy = pltpu.make_async_copy(
            source.at[:, pl.ds(lo, size)],
            o_ref.at[pl.ds(base + row, source.shape[0]), pl.ds(lo, size)],
            os.at[len(sent)],
        )
        copy.start()
        sent.append(copy)

    if ready:
        send(whole[0], ready, 0, width)
    for k, (row, i, at) in enumerate(tiles):
        mine = own_ref[:, base + row:base + row + tile]
        after = lambda lo: send(ob.at[k], row, lo, strip) if k >= fine else None
        multiply(mine, others[i][:, at:at + tile], g_ref, ob.at[k], strip, after)
        if k < fine:
            send(ob.at[k], row, 0, width)
    for copy in sent:
        copy.wait()


def local(grad_out, expert_ids, route_gates, saved_hidden):
    D, E, T = lax.axis_size("dp"), lax.axis_size("expert"), lax.axis_size("tensor")
    tokens, cols = grad_out.shape
    rows, units = saved_hidden.shape[1:]
    depth = D * E * CAP
    width = cols * T // D
    tile, strip = 256, 1024
    if (
        D != 2 or E & (E - 1) or E > 32 or T % D or cols % (128 * D) or units % (16 * tile) or width % strip
        or rows != E * CAP or tokens % 128
    ):
        return plain(grad_out, expert_ids, route_gates, saved_hidden)
    q = T // D
    hidden = saved_hidden[0]
    share = units // 16
    ahead, stop = EARLY * share, INSIDE * share
    done = READY * share
    later, at = [], stop
    for part in LATER:
        later.append((at, part * share))
        at += part * share
    later = tuple(later)
    vmem = pl.BlockSpec(memory_space=pltpu.VMEM)
    hbm = pl.BlockSpec(memory_space=pltpu.HBM)
    dma = pltpu.SemaphoreType.DMA
    bf16 = jnp.bfloat16
    swap = [(0, 1), (1, 0)]
    first = lax.ppermute(hidden[:, :ahead], "dp", swap)
    g, other, pre, *parts = pl.pallas_call(
        functools.partial(exchange, D, E, T, ahead, stop, done, tile, strip, later),
        out_shape=(
            pltpu.VMEM((depth, width), bf16),
            pltpu.VMEM((rows, stop - ahead), bf16),
            pltpu.VMEM((done, width), bf16),
            *(pltpu.VMEM((rows, size), bf16) for _, size in later),
        ),
        in_specs=[hbm] * 4,
        out_specs=(vmem, vmem, vmem, *(vmem for _ in later)),
        scratch_shapes=[
            pltpu.VMEM((TOP, tokens), jnp.int32),
            pltpu.VMEM((TOP, tokens), jnp.float32),
            pltpu.VMEM((tokens, cols), bf16),
            pltpu.VMEM((rows, stop - ahead), bf16),
            dma((4,)),
            pltpu.VMEM((E * CAP, cols), bf16),
            dma((len(later),)),
            dma((2,)), dma((2,)),
            dma((E, D)), dma((D, E)),
            dma((D - 1, D, E)), dma((D - 1, D, E)),
            dma((q - 1, D, D, E)), dma((q - 1, D, D, E)),
        ],
        cost_estimate=pl.CostEstimate(flops=2 * 10**10, bytes_accessed=2**22, transcendentals=0),
        compiler_params=pltpu.CompilerParams(has_side_effects=True, collective_id=0, vmem_limit_bytes=16777216),
    )(*(
        pltpu.with_memory_space_constraint(a, pltpu.HBM)
        for a in (expert_ids.T, route_gates.T, grad_out, hidden)
    ))
    arrived = []
    for part in parts:
        arrived.append(lax.ppermute(part, "dp", swap))

    def run(base, tiles, others, ready, pre, out):
        count = len(tiles)
        operands = (hidden, *others, g, *pre)
        return pl.pallas_call(
            functools.partial(product, base, tiles, ready, tile, strip),
            out_shape=jax.ShapeDtypeStruct((units, width), bf16),
            in_specs=[*(vmem for _ in operands), *(hbm for _ in out)],
            out_specs=hbm,
            scratch_shapes=[
                pltpu.VMEM((count, tile, width), bf16),
                dma((1 + count * (width // strip),)),
            ],
            compiler_params=pltpu.CompilerParams(vmem_limit_bytes=30 * 2**20),
            input_output_aliases={len(operands): 0} if out else {},
            cost_estimate=pl.CostEstimate(
                flops=2 * depth * width * count * tile,
                bytes_accessed=2 * width * count * tile,
                transcendentals=0,
            ),
        )(*operands, *out)

    tiles = [(at, 0, at) for at in range(0, ahead, tile)]
    tiles += [(at, 1, at - ahead) for at in range(ahead + done, stop, tile)]
    out = run(0, tiles, (first, other), ahead, (pre,), ())
    for (at, size), part in zip(later, arrived):
        out = run(at, [(k, 0, k) for k in range(0, size, tile)], (part,), 0, (), (out,))
    return out[None]


def solution(mesh):
    in_specs = (
        P(("dp", "expert"), "tensor"),
        P(("dp", "expert"), None),
        P(("dp", "expert"), None),
        P("expert", "dp", "tensor"),
    )
    out_specs = P("expert", "tensor", "dp")
    return jax.shard_map(local, mesh=mesh, in_specs=in_specs, out_specs=out_specs, check_vma=False)
```
